32 devices in a mesh: groups: 2 (over x), seq: 16 (over z, y, core).
Axes of the slice: x: 2, y: 2, z: 4, core: 2. Of those that a mesh axis runs over, the one named last changes fastest.
Arguments:
- queries: bfloat16 [8192, 4096], P(('groups', 'seq')), parts along dimension 0, may hold values from -6 to 6
- keys: bfloat16 [8192, 2048], P(('groups', 'seq')), parts along dimension 0, may hold values from -6 to 6
- values: bfloat16 [8192, 2048], P(('groups', 'seq')), parts along dimension 0, may hold values from -6 to 6
- doc_blocks: int32 [16], P('groups'), parts along dimension 0, may hold values from 1 to 8, 32 in all
Outputs:
- attended: bfloat16 [8192, 4096], P(('groups', 'seq')), parts along dimension 0
The draws below stay inside these ranges and needn't reach their ends.
There are 2 independent parts, one for each index of `groups`. The reference program is written for one: setup_inputs(seed, part) draws one part's arguments, and reference() takes and returns one part's arrays. A program takes and returns all parts, laid end to end along the dimension named above; each array names one. Nothing has to cross between parts.
Inputs may be any that keep to these rules, and one draw needn't show every extreme that they name: `doc_blocks`: the lengths add up to 32; the longest document has exactly 8 units.
All inputs are finite; a program needn't handle non-finite values.
Results may differ from the reference program's by a relative error of at most 0.004.
Values may be sent and summed in bfloat16 or wider, within the bound.
No kernel may reach another device: no remote copies, remote signals or barrier semaphores. Data moves between devices by JAX's collectives and lax.ppermute only.
A program may use at most 64 MiB of HBM per device.

```python
import math
import jax
import jax.numpy as jnp
import numpy as np
from jax import lax

HEADS = 32
KV_HEADS = 16
DH = 128
BLK = 128
DOCS = 8
TOKENS = 4096


def draw_keys(key, part):
    own_key = jax.random.fold_in(key, 11)
    background = jnp.clip(jax.random.normal(own_key, (TOKENS, KV_HEADS * DH), jnp.float32), -6.0, 6.0)
    return background.astype(jnp.bfloat16)


def draw_queries(key, part):
    own_key = jax.random.fold_in(key, 17)
    background = jnp.clip(jax.random.normal(own_key, (TOKENS, HEADS * DH), jnp.float32), -6.0, 6.0)
    return background.astype(jnp.bfloat16)


def levels(key, dims, pieces, low, high):
    def one(dim, shards_of):
        draws = jax.random.uniform(jax.random.fold_in(jax.random.fold_in(key, 6), dim), (shards_of,), jnp.float32, low / len(pieces), high / len(pieces))
        return jnp.repeat(jnp.exp(draws), dims[dim] // shards_of).reshape((-1,) + (1,) * (len(dims) - dim - 1))

    loudness = one(*pieces[0])
    for cut in pieces[1:]:
        loudness = loudness * one(*cut)
    return loudness


def length_profile(amount, total, most, slope):
    portions = [(1 << 20) // math.isqrt(rank ** slope) + 1 for rank in range(2, amount + 1)]
    spare, counts = total - most - (amount - 1), [1] * (amount - 1)
    while spare > 0:
        movable = [i for i in range(amount - 1) if counts[i] < most]
        mass, budget = sum([portions[i] for i in movable]), spare
        for i in movable:
            extra = min(most - counts[i], max(1, budget * portions[i] // mass), spare)
            counts[i] = counts[i] + extra
            spare = spare - extra
    return np.array([most] + counts)


def ragged_sizes(stream_key, number_of, total, limit, lean):
    if number_of == 2:
        one = jax.random.randint(stream_key, (), max(1, total - limit), min(limit, total - 1) + 1)
        return jnp.stack([one, total - one])
    tallies = jnp.asarray(length_profile(number_of, total, limit, lean), jnp.int32)
    twos = (number_of - 1) // 2
    source_of, sink = tallies[1:1 + 2 * twos:2], tallies[2:2 + 2 * twos:2]
    margin = jnp.minimum(source_of - 1, limit - sink)
    shifted = jax.random.randint(jax.random.fold_in(stream_key, 1), (twos,), 0, 1 << 20) % (margin + 1)
    tallies = tallies.at[1:1 + 2 * twos:2].set(source_of - shifted).at[2:2 + 2 * twos:2].set(sink + shifted)
    return tallies[jax.random.permutation(jax.random.fold_in(stream_key, 2), number_of)]


def bell_draw(key, dims, width, most, pieces=(), held_as=jnp.bfloat16):
    gain = levels(key, dims, pieces, -0.22, 0.18) if pieces else 1.0
    entries = jax.random.normal(key, dims, jnp.float32) * width * gain
    return jnp.minimum(jnp.maximum(entries, -most), most).astype(held_as)


def setup_inputs(seed: int = 0, part: int = 0) -> dict:
    key_list = jax.random.split(jax.random.key(seed), 5)
    own_keys = jax.random.split(jax.random.fold_in(key_list[4], part), 5)
    queries = draw_queries(jax.random.fold_in(jax.random.fold_in(key_list[4], part), 71), part)
    keys = draw_keys(jax.random.fold_in(jax.random.fold_in(key_list[4], part), 71), part)
    values = bell_draw(own_keys[2], (TOKENS, KV_HEADS * DH), 1.0, 6.0, ((0, 16),))
    doc_blocks = ragged_sizes(own_keys[3], DOCS, TOKENS // BLK, TOKENS // BLK // 4, 2).astype(jnp.int32)
    return dict(queries=queries, keys=keys, values=values, doc_blocks=doc_blocks)


score_scale = 144.0 ** -0.5


def reference(queries, keys, values, doc_blocks):
    lengths = doc_blocks.astype(jnp.int32) * BLK
    doc_ends = jnp.cumsum(lengths).astype(jnp.int32)
    doc_starts = (doc_ends - lengths).astype(jnp.int32)
    positions = jnp.arange(TOKENS, dtype=jnp.int32)
    doc_number = jnp.sum((positions[:, None] >= doc_ends[None, :]).astype(jnp.int32), axis=1).astype(jnp.int32)
    own_start = jnp.sum(jnp.where(doc_number[:, None] == jnp.arange(DOCS, dtype=jnp.int32)[None, :], doc_starts[None, :], 0), axis=1).astype(jnp.int32)
    query_heads = queries.reshape(TOKENS, KV_HEADS, HEADS // KV_HEADS, DH)
    key_heads = keys.reshape(TOKENS, KV_HEADS, DH)
    value_heads = values.reshape(TOKENS, KV_HEADS, DH)
    tile_rows = min(256, TOKENS)
    window_rows = min(TOKENS, TOKENS // 4 + tile_rows)

    def one_tile(block_index):
        first_row = (block_index * tile_rows).astype(jnp.int32)
        query_tile = lax.dynamic_slice_in_dim(query_heads, first_row, tile_rows, 0).astype(jnp.float32)
        key_first = jnp.clip(first_row + tile_rows - window_rows, 0, TOKENS - window_rows).astype(jnp.int32)
        key_tile = lax.dynamic_slice_in_dim(key_heads, key_first, window_rows, 0).astype(jnp.float32)
        value_tile = lax.dynamic_slice_in_dim(value_heads, key_first, window_rows, 0).astype(jnp.float32)
        scores = jnp.einsum("qgsd,kgd->gsqk", query_tile, key_tile) * score_scale
        tile_pos = first_row + jnp.arange(tile_rows, dtype=jnp.int32)
        tile_start = lax.dynamic_slice_in_dim(own_start, first_row, tile_rows, 0)
        key_pos = key_first + jnp.arange(window_rows, dtype=jnp.int32)
        visible = (key_pos[None, :] >= tile_start[:, None]) & (key_pos[None, :] <= tile_pos[:, None])
        row_max = jnp.max(jnp.where(visible, scores, -1e30), axis=-1)
        weights = jnp.where(visible, jnp.exp(scores - row_max[..., None]), 0.0)
        row_total = jnp.sum(weights, axis=-1)
        rounded = lax.optimization_barrier(weights.astype(jnp.bfloat16)).astype(jnp.float32)
        blended = jnp.einsum("gsqk,kgd->gsqd", rounded, value_tile) / row_total[..., None]
        return blended.transpose(2, 0, 1, 3).reshape(tile_rows, HEADS * DH).astype(jnp.bfloat16)

    blocks = lax.map(one_tile, jnp.arange(TOKENS // tile_rows, dtype=jnp.int32))
    return blocks.reshape(TOKENS, HEADS * DH)
```

```python
import functools
import math

import jax
import jax.numpy as jnp
from jax import lax
from jax.experimental import pallas as pl
from jax.experimental.pallas import tpu as pltpu
from jax.sharding import PartitionSpec as P

DH = 128
BLK = 128
CORES = 2
SCALE = 144.0 ** (-0.5)


def shift(block, pairs):
    return lax.ppermute(block, "seq", pairs)


def attend_kernel(
    plan,
    blocks,
    q_own,
    q_far,
    k_own,
    v_own,
    kv_far,
    *rest,
):
    first, heads, half, ratio, window, spans = plan
    befores = rest[:spans]
    rest = rest[spans:]
    if first > 0:
        rest = rest[1:]
    out, out_far, q_buf, k_buf, v_buf, o_buf, sems = rest
    rows = q_own.shape[0]
    chip_rows = rows * CORES
    me = lax.axis_index("seq")
    core = me % CORES
    chip = me // CORES
    kv_width = heads * DH
    q_width = kv_width * ratio
    base = spans * chip_rows
    kv_col = pl.multiple_of((core * half + first) * DH, DH)
    q_col = pl.multiple_of((core * half + first) * DH * ratio, DH)
    mine = pl.multiple_of(core * rows, rows)
    other = pl.multiple_of((1 - core) * rows, rows)

    copies = []

    def load(src, dst):
        copy = pltpu.make_async_copy(src, dst, sems.at[len(copies)])
        copy.start()
        copies.append(copy)

    load(q_own.at[:, pl.ds(q_col, q_width)], q_buf.at[pl.ds(mine, rows)])
    load(q_far.at[:, pl.ds(first * DH * ratio, q_width)], q_buf.at[pl.ds(other, rows)])
    load(k_own.at[:, pl.ds(kv_col, kv_width)], k_buf.at[pl.ds(base + mine, rows)])
    load(v_own.at[:, pl.ds(kv_col, kv_width)], v_buf.at[pl.ds(base + mine, rows)])
    far_cols = pl.ds(first * DH, kv_width)
    load(kv_far.at[0, :, far_cols], k_buf.at[pl.ds(base + other, rows)])
    load(kv_far.at[1, :, far_cols], v_buf.at[pl.ds(base + other, rows)])
    for distance in range(1, spans + 1):
        piece = befores[distance - 1]
        at = base - distance * chip_rows
        load(piece.at[0, 0], k_buf.at[pl.ds(at + mine, rows)])
        load(piece.at[0, 1], v_buf.at[pl.ds(at + mine, rows)])
        load(piece.at[1, 0], k_buf.at[pl.ds(at + other, rows)])
        load(piece.at[1, 1], v_buf.at[pl.ds(at + other, rows)])
    for copy in copies:
        copy.wait()

    units = chip_rows // BLK
    keys_seen = window * BLK
    factor = SCALE * math.log2(math.e)

    def one_tile(step, carry):
        group = step // units
        unit = step % units
        number = chip * units + unit
        begin = jnp.int32(0)
        total = jnp.int32(0)
        for doc in range(blocks.shape[0]):
            begin = jnp.where(number >= total, total, begin)
            total = total + blocks[doc]
        hidden = (window - 1 - (number - begin)) * BLK
        q_at = pl.ds(pl.multiple_of(unit * BLK, BLK), BLK)
        kv_cols = pl.ds(pl.multiple_of(group * DH, DH), DH)
        kv_at = pl.ds(pl.multiple_of(base + (unit - (window - 1)) * BLK, BLK), keys_seen)
        tiles = [
            q_buf[q_at, pl.ds(pl.multiple_of((group * ratio + s) * DH, DH), DH)]
            for s in range(ratio)
        ]
        tile = jnp.concatenate(tiles, axis=0)
        scores = lax.dot_general(
            tile,
            k_buf[kv_at, kv_cols],
            (((1,), (1,)), ((), ())),
            preferred_element_type=jnp.float32,
        )
        key = lax.broadcasted_iota(jnp.int32, (BLK, keys_seen), 1)
        row = lax.broadcasted_iota(jnp.int32, (BLK, keys_seen), 0)
        visible = (key >= hidden) & (key - (keys_seen - BLK) <= row)
        visible = jnp.concatenate([visible] * ratio, axis=0)
        scores = jnp.where(visible, scores, -1e30)
        top = jnp.max(scores, axis=1, keepdims=True)
        weights = jnp.exp2((scores - top) * factor)
        row_total = jnp.sum(weights, axis=1, keepdims=True)
        blended = jnp.dot(
            weights.astype(jnp.bfloat16),
            v_buf[kv_at, kv_cols],
            preferred_element_type=jnp.float32,
        )
        blended = (blended / row_total).astype(jnp.bfloat16)
        for s in range(ratio):
            cols = pl.ds(pl.multiple_of((group * ratio + s) * DH, DH), DH)
            o_buf[q_at, cols] = blended[s * BLK : (s + 1) * BLK]
        return carry

    lax.fori_loop(0, heads * units, one_tile, 0)
    far = pltpu.make_async_copy(o_buf.at[pl.ds(other, rows)], out_far, sems.at[0])
    near = pltpu.make_async_copy(
        o_buf.at[pl.ds(mine, rows)], out.at[:, pl.ds(q_col, q_width)], sems.at[1]
    )
    far.start()
    near.start()
    far.wait()
    near.wait()


def attend(plan, blocks, q_own, q_far, k_own, v_own, kv_far, befores, out):
    first, heads, half, ratio, window, spans = plan
    rows = q_own.shape[0]
    chip_rows = rows * CORES
    held = (spans + 1) * chip_rows
    kv_width = heads * DH
    q_width = kv_width * ratio
    anywhere = pl.BlockSpec(memory_space=pl.ANY)
    arguments = [blocks, q_own, q_far, k_own, v_own, kv_far, *befores]
    aliases = {}
    if out is not None:
        aliases = {len(arguments): 0}
        arguments.append(out)
    copies = 6 + 4 * spans
    scores = heads * ratio * chip_rows * window * BLK
    return pl.pallas_call(
        functools.partial(attend_kernel, plan),
        out_shape=(
            jax.ShapeDtypeStruct(q_own.shape, q_own.dtype),
            jax.ShapeDtypeStruct((rows, q_width), q_own.dtype),
        ),
        in_specs=[pl.BlockSpec(memory_space=pltpu.SMEM)] + [anywhere] * (len(arguments) - 1),
        out_specs=(anywhere, anywhere),
        scratch_shapes=[
            pltpu.VMEM((chip_rows, q_width), jnp.bfloat16),
            pltpu.VMEM((held, kv_width), jnp.bfloat16),
            pltpu.VMEM((held, kv_width), jnp.bfloat16),
            pltpu.VMEM((chip_rows, q_width), jnp.bfloat16),
            pltpu.SemaphoreType.DMA((copies,)),
        ],
        input_output_aliases=aliases,
        cost_estimate=pl.CostEstimate(
            flops=4 * scores * DH,
            bytes_accessed=2 * (chip_rows * q_width * 2 + held * kv_width * 2),
            transcendentals=scores,
        ),
        name=f"attend_{first}",
    )(*arguments)


def place_kernel(firsts, half, ratio, *refs):
    pieces = refs[: len(firsts)]
    out = refs[len(firsts) + 1]
    buffers = refs[len(firsts) + 2 : -2]
    sems_in, sems_out = refs[-2:]
    core = lax.axis_index("seq") % CORES
    loads = [
        pltpu.make_async_copy(piece, buffer, sems_in.at[i])
        for i, (piece, buffer) in enumerate(zip(pieces, buffers))
    ]
    for load in loads:
        load.start()
    stores = []
    for i, first in enumerate(firsts):
        col = pl.multiple_of(((1 - core) * half + first) * ratio * DH, DH)
        loads[i].wait()
        store = pltpu.make_async_copy(
            buffers[i], out.at[:, pl.ds(col, buffers[i].shape[1])], sems_out.at[i]
        )
        store.start()
        stores.append(store)
    for store in stores:
        store.wait()


def place(firsts, half, ratio, pieces, out):
    anywhere = pl.BlockSpec(memory_space=pl.ANY)
    return pl.pallas_call(
        functools.partial(place_kernel, firsts, half, ratio),
        out_shape=jax.ShapeDtypeStruct(out.shape, out.dtype),
        in_specs=[anywhere] * (len(pieces) + 1),
        out_specs=anywhere,
        scratch_shapes=[pltpu.VMEM(piece.shape, piece.dtype) for piece in pieces]
        + [pltpu.SemaphoreType.DMA((len(pieces),))] * 2,
        input_output_aliases={len(pieces): 0},
        name="place",
    )(*pieces, out)


def chunk_heads(half):
    sizes = []
    left = half
    while left > 2:
        sizes.append(2)
        left -= 2
    sizes += [1] * left
    return sizes


def on_device(queries, keys, values, doc_blocks):
    devices = lax.axis_size("seq")
    me = lax.axis_index("seq")
    rows = queries.shape[0]
    q_heads = queries.shape[1] // DH
    kv_heads = keys.shape[1] // DH
    ratio = q_heads // kv_heads
    half = kv_heads // CORES
    chips = devices // CORES
    chip_rows = rows * CORES
    core = me % CORES
    row_of_pair = me // CORES % 2
    window = rows * devices // BLK // 4
    spans = min(-(-(window - 1) * BLK // chip_rows), chips)

    partner = [(i, i ^ 1) for i in range(devices)]
    next_chip = [(i, i + CORES) for i in range(devices - CORES)]
    next_pair = [(i, i + 2 * CORES) for i in range(devices - 2 * CORES)]
    across = [(i, i ^ CORES) for i in range(devices)]
    paired = spans == 2 and chips % 2 == 0

    def half_of(array, which, width):
        return lax.dynamic_slice_in_dim(array, which * half * width, half * width, 1)

    kv_far = shift(
        jnp.stack([half_of(keys, 1 - core, DH), half_of(values, 1 - core, DH)]), partner
    )
    q_far = shift(half_of(queries, 1 - core, DH * ratio), partner)

    sizes = chunk_heads(half)
    firsts = [sum(sizes[:i]) for i in range(len(sizes))]

    def packed(first, heads):
        col = (core * half + first) * DH
        own = jnp.stack(
            [lax.dynamic_slice_in_dim(array, col, heads * DH, 1) for array in (keys, values)]
        )
        return jnp.stack([own, kv_far[:, :, first * DH : (first + heads) * DH]])

    out = None
    pieces = []
    for first, heads in zip(firsts, sizes):
        own = packed(first, heads)
        befores = []
        if paired:
            two_back = shift(own, next_pair)
            one_back = shift(jnp.where(row_of_pair == 0, own, two_back), across)
            befores = [one_back, two_back]
        else:
            moved = own
            for _ in range(spans):
                moved = shift(moved, next_chip)
                befores.append(moved)
        plan = (first, heads, half, ratio, window, spans)
        out, out_far = attend(
            plan, doc_blocks, queries, q_far, keys, values, kv_far, befores, out
        )
        pieces.append(shift(out_far, partner))
    return place(firsts, half, ratio, pieces, out)


def solution(mesh):
    spec = P(("groups", "seq"), None)
    return jax.shard_map(
        on_device,
        mesh=mesh,
        in_specs=(spec, spec, spec, P("groups")),
        out_specs=spec,
        check_vma=False,
    )
```

```python
import functools
import math

import jax
import jax.numpy as jnp
from jax import lax
from jax.experimental import pallas as pl
from jax.experimental.pallas import tpu as pltpu
from jax.sharding import PartitionSpec as P


DH = 128
BLK = 128
CORES = 2
BUCKETS = 4
PART = 32
SCALE = 144.0 ** (-0.5)


def shift(block, pairs):
    return lax.ppermute(block, "seq", pairs)


def attend_kernel(plan, blocks, q_near, q_far, *rest):
    first, heads, _, ratio, window, spans = plan
    pieces = rest[: spans + 1]
    out_near, out_far, q_buf, k_buf, v_buf, o_buf, s_buf, w_buf = rest[spans + 1 :]
    rows = q_near.shape[-2]
    chip_rows = rows * CORES
    me = lax.axis_index("seq")
    core = me % CORES
    chip = me // CORES
    q_width = heads * DH * ratio
    base = spans * chip_rows
    q_cols = slice(first * DH * ratio, first * DH * ratio + q_width)
    mine = pl.multiple_of(core * rows, rows)
    other = pl.multiple_of((1 - core) * rows, rows)
    q_buf[pl.ds(mine, rows)] = q_near[0, :, q_cols]
    q_buf[pl.ds(other, rows)] = q_far[0, :, q_cols]
    for distance in range(spans + 1):
        at = slice(base - distance * chip_rows, base - distance * chip_rows + chip_rows)
        k_buf[at] = pieces[distance][0]
        v_buf[at] = pieces[distance][1]

    units = chip_rows // BLK
    factor = SCALE * math.log2(math.e)
    tile_rows = ratio * BLK

    def one_tile(step, carry):
        group = step // units
        unit = step % units
        number = chip * units + unit
        begin = jnp.int32(0)
        total = jnp.int32(0)
        for doc in range(blocks.shape[0]):
            begin = jnp.where(number >= total, total, begin)
            total = total + blocks[doc]
        count = number - begin + 1
        q_at = pl.ds(pl.multiple_of(unit * BLK, BLK), BLK)
        kv_cols = pl.ds(pl.multiple_of(group * DH, DH), DH)

        def with_keys(shown):
            keys_seen = shown * BLK
            kv_at = pl.ds(pl.multiple_of(base + (unit + 1 - shown) * BLK, BLK), keys_seen)
            tiles = [
                q_buf[q_at, pl.ds(pl.multiple_of((group * ratio + s) * DH, DH), DH)]
                for s in range(ratio)
            ]
            s_buf[:, :keys_seen] = lax.dot_general(
                jnp.concatenate(tiles, axis=0),
                k_buf[kv_at, kv_cols],
                (((1,), (1,)), ((), ())),
                preferred_element_type=jnp.float32,
            )
            hidden = (shown - count) * BLK
            unsure = min(step_units, shown) * BLK
            key = lax.broadcasted_iota(jnp.int32, (PART, unsure), 1)
            totals = []
            for part in range(tile_rows // PART):
                at = slice(part * PART, (part + 1) * PART)
                scores = s_buf[at, :keys_seen]
                front = jnp.where(key >= hidden, scores[:, :unsure], -1e30)
                if unsure < keys_seen:
                    scores = jnp.concatenate([front, scores[:, unsure:]], axis=1)
                else:
                    scores = front
                last = lax.broadcasted_iota(jnp.int32, (PART, BLK), 1)
                row = lax.broadcasted_iota(jnp.int32, (PART, BLK), 0) + part * PART % BLK
                tail = jnp.where(last <= row, scores[:, keys_seen - BLK :], -1e30)
                if keys_seen > BLK:
                    scores = jnp.concatenate([scores[:, : keys_seen - BLK], tail], axis=1)
                else:
                    scores = tail
                top = jnp.max(scores, axis=1, keepdims=True) * factor
                weights = jnp.exp2(scores * factor - top)
                totals.append(jnp.sum(weights, axis=1, keepdims=True))
                w_buf[at, :keys_seen] = weights.astype(jnp.bfloat16)
            blended = jnp.dot(
                w_buf[:, :keys_seen],
                v_buf[kv_at, kv_cols],
                preferred_element_type=jnp.float32,
            )
            blended = (blended / jnp.concatenate(totals, axis=0)).astype(jnp.bfloat16)
            for s in range(ratio):
                cols = pl.ds(pl.multiple_of((group * ratio + s) * DH, DH), DH)
                o_buf[q_at, cols] = blended[s * BLK : (s + 1) * BLK]

        step_units = -(-window // BUCKETS)
        shown = 0
        while shown < window:
            lower, shown = shown, min(shown + step_units, window)
            pl.when((count > lower) & (count <= shown))(functools.partial(with_keys, shown))
        return carry

    lax.fori_loop(0, heads * units, one_tile, 0)
    out_near[...] = o_buf[pl.ds(mine, rows)]
    out_far[...] = o_buf[pl.ds(other, rows)]


def attend(plan, blocks, q_near, q_far, pieces):
    _, heads, _, ratio, window, spans = plan
    rows = q_near.shape[-2]
    chip_rows = rows * CORES
    held = (spans + 1) * chip_rows
    kv_width = heads * DH
    q_width = kv_width * ratio
    scores = heads * ratio * chip_rows * window * BLK
    scratch_bytes = (chip_rows * q_width + held * kv_width) * 4 + ratio * BLK * window * BLK * 6
    near_by = pl.BlockSpec(memory_space=pltpu.VMEM)
    shape = pltpu.VMEM((rows, q_width), q_near.dtype)
    return pl.pallas_call(
        functools.partial(attend_kernel, plan),
        out_shape=(shape, shape),
        in_specs=[pl.BlockSpec(memory_space=pltpu.SMEM)] + [near_by] * (2 + len(pieces)),
        out_specs=(near_by, near_by),
        scratch_shapes=[
            pltpu.VMEM((chip_rows, q_width), jnp.bfloat16),
            pltpu.VMEM((held, kv_width), jnp.bfloat16),
            pltpu.VMEM((held, kv_width), jnp.bfloat16),
            pltpu.VMEM((chip_rows, q_width), jnp.bfloat16),
            pltpu.VMEM((ratio * BLK, window * BLK), jnp.float32),
            pltpu.VMEM((ratio * BLK, window * BLK), jnp.bfloat16),
        ],
        cost_estimate=pl.CostEstimate(
            flops=4 * scores * DH,
            bytes_accessed=2 * (chip_rows * q_width * 2 + held * kv_width * 2),
            transcendentals=scores,
        ),
        compiler_params=pltpu.CompilerParams(vmem_limit_bytes=scratch_bytes + (6 << 20)),
    )(blocks, q_near, q_far, *pieces)


def place_kernel(firsts, half, ratio, *refs):
    count = len(firsts)
    out, sems = refs[2 * count :]
    core = lax.axis_index("seq") % CORES
    stores = []
    for i, first in enumerate(firsts):
        for which, piece in ((core, refs[i]), (1 - core, refs[count + i])):
            col = pl.multiple_of((which * half + first) * ratio * DH, DH)
            store = pltpu.make_async_copy(
                piece, out.at[:, pl.ds(col, piece.shape[1])], sems.at[len(stores)]
            )
            store.start()
            stores.append(store)
    for store in stores:
        store.wait()


def place(firsts, half, ratio, nears, fars, width):
    anywhere = pl.BlockSpec(memory_space=pl.ANY)
    return pl.pallas_call(
        functools.partial(place_kernel, firsts, half, ratio),
        out_shape=pltpu.HBM((nears[0].shape[0], width), nears[0].dtype),
        in_specs=[anywhere] * (2 * len(firsts)),
        out_specs=anywhere,
        scratch_shapes=[pltpu.SemaphoreType.DMA((2 * len(firsts),))],
        compiler_params=pltpu.CompilerParams(vmem_limit_bytes=1 << 20),
        name="place",
    )(*nears, *fars)


def split_kernel(arrays, widths, *refs):
    sources, far, near, sems = refs[:arrays], *refs[arrays:]
    core = lax.axis_index("seq") % CORES
    copies = []
    for which, target in ((1 - core, far), (core, near)):
        for i in range(arrays):
            col = pl.multiple_of(which * widths, DH)
            copy = pltpu.make_async_copy(
                sources[i].at[:, pl.ds(col, widths)], target.at[i], sems.at[len(copies)]
            )
            copy.start()
            copies.append(copy)
    for copy in copies:
        copy.wait()


def split(*arrays):
    rows, columns = arrays[0].shape
    width = columns // CORES
    shape = pltpu.VMEM((len(arrays), rows, width), arrays[0].dtype)
    anywhere = pl.BlockSpec(memory_space=pl.ANY)
    return pl.pallas_call(
        functools.partial(split_kernel, len(arrays), width),
        out_shape=(shape, shape),
        in_specs=[pl.BlockSpec(memory_space=pltpu.HBM)] * len(arrays),
        out_specs=(anywhere, anywhere),
        scratch_shapes=[pltpu.SemaphoreType.DMA((CORES * len(arrays),))],
        compiler_params=pltpu.CompilerParams(vmem_limit_bytes=1 << 20),
        name="split",
    )(*arrays)


def merge_kernel(sizes, near, far, *outs):
    core = lax.axis_index("seq") % CORES
    rows = near.shape[1]
    mine = pl.multiple_of(core * rows, rows)
    other = pl.multiple_of((1 - core) * rows, rows)
    col = 0
    for heads, out in zip(sizes, outs):
        cols = slice(col, col + heads * DH)
        out[:, pl.ds(mine, rows)] = near[:, :, cols]
        out[:, pl.ds(other, rows)] = far[:, :, cols]
        col += heads * DH


def merge(sizes, near, far):
    arrays, rows, _ = near.shape
    near_by = pl.BlockSpec(memory_space=pltpu.VMEM)
    return pl.pallas_call(
        functools.partial(merge_kernel, sizes),
        out_shape=tuple(
            pltpu.VMEM((arrays, rows * CORES, heads * DH), near.dtype) for heads in sizes
        ),
        in_specs=[near_by, near_by],
        out_specs=(near_by,) * len(sizes),
        compiler_params=pltpu.CompilerParams(vmem_limit_bytes=12 << 20),
        name="merge",
    )(near, far)


def choose_kernel(own, came, out):
    row = lax.axis_index("seq") // CORES % 2

    @pl.when(row == 0)
    def _():
        out[...] = own[...]

    @pl.when(row == 1)
    def _():
        out[...] = came[...]


def choose(own, came):
    near_by = pl.BlockSpec(memory_space=pltpu.VMEM)
    return pl.pallas_call(
        choose_kernel,
        out_shape=pltpu.VMEM(own.shape, own.dtype),
        in_specs=[near_by, near_by],
        out_specs=near_by,
        compiler_params=pltpu.CompilerParams(vmem_limit_bytes=6 << 20),
        name="choose",
    )(own, came)


def chunk_heads(half):
    sizes = [2] * (half // 2)
    return sizes + [1] * (half % 2)


def on_device(queries, keys, values, doc_blocks):
    devices = lax.axis_size("seq")
    rows = queries.shape[0]
    q_heads = queries.shape[1] // DH
    kv_heads = keys.shape[1] // DH
    ratio = q_heads // kv_heads
    half = kv_heads // CORES
    chips = devices // CORES
    chip_rows = rows * CORES
    window = rows * devices // BLK // 4
    spans = min(-(-(window - 1) * BLK // chip_rows), chips)

    partner = [(i, i ^ 1) for i in range(devices)]
    next_chip = [(i, i + CORES) for i in range(devices - CORES)]
    next_pair = [(i, i + 2 * CORES) for i in range(devices - 2 * CORES)]
    across = [(i, i ^ CORES) for i in range(devices)]
    paired = spans == 2 and chips % 2 == 0

    kv_send, kv_near = split(keys, values)
    kv_far = shift(kv_send, partner)
    q_send, q_near = split(queries)
    q_far = shift(q_send, partner)

    sizes = chunk_heads(half)
    firsts = [sum(sizes[:i]) for i in range(len(sizes))]

    nears, fars = [], []
    for first, heads, own in zip(firsts, sizes, merge(sizes, kv_near, kv_far)):
        held = [own]
        if paired:
            two_back = shift(own, next_pair)
            chosen = choose(own, two_back)
            one_back = shift(chosen, across)
            held += [one_back, two_back]
        else:
            for _ in range(spans):
                held.append(shift(held[-1], next_chip))
        plan = (first, heads, half, ratio, window, spans)
        out_near, out_far = attend(plan, doc_blocks, q_near, q_far, held)
        nears.append(out_near)
        fars.append(shift(out_far, partner))
    return place(firsts, half, ratio, nears, fars, queries.shape[1])


def solution(mesh):
    spec = P(("groups", "seq"), None)

    return jax.shard_map(
        on_device,
        mesh=mesh,
        in_specs=(spec, spec, spec, P("groups")),
        out_specs=spec,
        check_vma=False,
    )
```

```python
import functools
import math

import jax
import jax.numpy as jnp
from jax import lax
from jax.experimental import pallas as pl
from jax.experimental.pallas import tpu as pltpu
from jax.sharding import PartitionSpec as P


DH = 128
BLK = 128
CORES = 2
SLOTS = 4
PART = 16
SCALE = 144.0 ** (-0.5)


def shift(block, pairs):
    return lax.ppermute(block, "seq", pairs)


def attend_kernel(plan, spots, blocks, q_near, q_far, *rest):
    first, heads, _, ratio, window, spans = plan
    pieces = rest[: len(spots)]
    out_near, out_far, q_buf, k_buf, v_buf, o_buf, s_buf, w_buf = rest[len(spots) :]
    rows = q_near.shape[-2]
    chip_rows = rows * CORES
    me = lax.axis_index("seq")
    core = me % CORES
    chip = me // CORES
    q_width = heads * DH * ratio
    base = spans * chip_rows
    q_cols = slice(first * DH * ratio, first * DH * ratio + q_width)
    mine = pl.multiple_of(core * rows, rows)
    other = pl.multiple_of((1 - core) * rows, rows)
    q_buf[pl.ds(mine, rows)] = q_near[0, :, q_cols]
    q_buf[pl.ds(other, rows)] = q_far[0, :, q_cols]

    def bring(piece, at, col):
        k_buf[at : at + piece.shape[1]] = piece[0, :, col : col + heads * DH]
        v_buf[at : at + piece.shape[1]] = piece[1, :, col : col + heads * DH]

    for piece, (at, col, side) in zip(pieces, spots):
        if side is None:
            bring(piece, at, col)
        else:
            pl.when(chip % 2 == side)(functools.partial(bring, piece, at, col))

    units = chip_rows // BLK
    factor = SCALE * math.log2(math.e)
    tile_rows = ratio * BLK
    keys_seen = window * BLK
    last = lax.broadcasted_iota(jnp.int32, (BLK, BLK), 1)
    row = lax.broadcasted_iota(jnp.int32, (BLK, BLK), 0)
    causal = jnp.where(last <= row, 0.0, -1e30)
    key = lax.broadcasted_iota(jnp.int32, (8, keys_seen - BLK), 1)
    ones = jnp.ones((keys_seen, DH), jnp.bfloat16)

    def keys_of(unit):
        first_key = base + (unit + 1 - window) * BLK
        return pl.ds(first_key, keys_seen)

    def score(unit, group):
        q_at = pl.ds(unit * BLK, BLK)
        tiles = [
            q_buf[q_at, (group * ratio + s) * DH : (group * ratio + s + 1) * DH]
            for s in range(ratio)
        ]
        s_buf[(unit * heads + group) % SLOTS] = lax.dot_general(
            jnp.concatenate(tiles, axis=0),
            k_buf[keys_of(unit), group * DH : (group + 1) * DH],
            (((1,), (1,)), ((), ())),
            preferred_element_type=jnp.float32,
        )

    def weigh(unit, group):
        number = chip * units + unit
        begin = jnp.int32(0)
        total = jnp.int32(0)
        for doc in range(blocks.shape[0]):
            begin = jnp.where(number >= total, total, begin)
            total = total + blocks[doc]
        hidden = (window - 1 - number + begin) * BLK
        before = jnp.where(key >= hidden, 0.0, -1e30)
        before = jnp.concatenate([before] * (PART // 8), axis=0)
        slot = (unit * heads + group) % SLOTS
        for part in range(tile_rows // PART):
            at = slice(part * PART, (part + 1) * PART)
            low = part * PART % BLK
            bias = jnp.concatenate([before, causal[low : low + PART]], axis=1)
            scores = s_buf[slot, at] * factor + bias
            top = jnp.max(scores, axis=1, keepdims=True)
            w_buf[slot, at] = jnp.exp2(scores - top).astype(jnp.bfloat16)

    def blend(unit, group):
        v_part = v_buf[keys_of(unit), group * DH : (group + 1) * DH]
        blended = jnp.dot(
            w_buf[(unit * heads + group) % SLOTS],
            jnp.concatenate([v_part, ones], axis=1),
            preferred_element_type=jnp.float32,
        )
        blended = (blended[:, :DH] / blended[:, DH:]).astype(jnp.bfloat16)
        for s in range(ratio):
            cols = slice((group * ratio + s) * DH, (group * ratio + s + 1) * DH)
            o_buf[pl.ds(unit * BLK, BLK), cols] = blended[s * BLK : (s + 1) * BLK]

    tiles = [(unit, group) for unit in range(units) for group in range(heads)]
    for step in range(len(tiles) + 2):
        if step < len(tiles):
            score(*tiles[step])
        if 0 <= step - 1 < len(tiles):
            weigh(*tiles[step - 1])
        if 0 <= step - 2:
            blend(*tiles[step - 2])
    out_near[...] = o_buf[pl.ds(mine, rows)]
    out_far[...] = o_buf[pl.ds(other, rows)]


def attend(plan, spots, blocks, q_near, q_far, pieces):
    _, heads, _, ratio, window, spans = plan
    rows = q_near.shape[-2]
    chip_rows = rows * CORES
    held = (spans + 1) * chip_rows
    kv_width = heads * DH
    q_width = kv_width * ratio
    scores = heads * ratio * chip_rows * window * BLK
    scratch_bytes = (chip_rows * q_width + held * kv_width) * 4 + SLOTS * ratio * BLK * window * BLK * 6
    near_by = pl.BlockSpec(memory_space=pltpu.VMEM)
    shape = pltpu.VMEM((rows, q_width), q_near.dtype)
    return pl.pallas_call(
        functools.partial(attend_kernel, plan, spots),
        out_shape=(shape, shape),
        in_specs=[pl.BlockSpec(memory_space=pltpu.SMEM)] + [near_by] * (2 + len(pieces)),
        out_specs=(near_by, near_by),
        scratch_shapes=[
            pltpu.VMEM((chip_rows, q_width), jnp.bfloat16),
            pltpu.VMEM((held, kv_width), jnp.bfloat16),
            pltpu.VMEM((held, kv_width), jnp.bfloat16),
            pltpu.VMEM((chip_rows, q_width), jnp.bfloat16),
            pltpu.VMEM((SLOTS, ratio * BLK, window * BLK), jnp.float32),
            pltpu.VMEM((SLOTS, ratio * BLK, window * BLK), jnp.bfloat16),
        ],
        cost_estimate=pl.CostEstimate(
            flops=4 * scores * DH,
            bytes_accessed=2 * (chip_rows * q_width * 2 + held * kv_width * 2),
            transcendentals=scores,
        ),
        compiler_params=pltpu.CompilerParams(vmem_limit_bytes=scratch_bytes + (6 << 20)),
    )(blocks, q_near, q_far, *pieces)


def place_kernel(firsts, half, ratio, *refs):
    count = len(firsts)
    out, sems = refs[2 * count :]
    core = lax.axis_index("seq") % CORES
    stores = []
    for i, first in enumerate(firsts):
        for which, piece in ((core, refs[i]), (1 - core, refs[count + i])):
            col = pl.multiple_of((which * half + first) * ratio * DH, DH)
            store = pltpu.make_async_copy(
                piece, out.at[:, pl.ds(col, piece.shape[1])], sems.at[len(stores)]
            )
            store.start()
            stores.append(store)
    for store in stores:
        store.wait()


def place(firsts, half, ratio, nears, fars, width):
    anywhere = pl.BlockSpec(memory_space=pl.ANY)
    return pl.pallas_call(
        functools.partial(place_kernel, firsts, half, ratio),
        out_shape=pltpu.HBM((nears[0].shape[0], width), nears[0].dtype),
        in_specs=[anywhere] * (2 * len(firsts)),
        out_specs=anywhere,
        scratch_shapes=[pltpu.SemaphoreType.DMA((2 * len(firsts),))],
        compiler_params=pltpu.CompilerParams(vmem_limit_bytes=1 << 20),
        name="place",
    )(*nears, *fars)


def split_kernel(arrays, widths, *refs):
    sources, far, near, sems = refs[:arrays], *refs[arrays:]
    core = lax.axis_index("seq") % CORES
    copies = []
    for which, target in ((1 - core, far), (core, near)):
        for i in range(arrays):
            col = pl.multiple_of(which * widths, DH)
            copy = pltpu.make_async_copy(
                sources[i].at[:, pl.ds(col, widths)], target.at[i], sems.at[len(copies)]
            )
            copy.start()
            copies.append(copy)
    for copy in copies:
        copy.wait()


def split(*arrays):
    rows, columns = arrays[0].shape
    width = columns // CORES
    shape = pltpu.VMEM((len(arrays), rows, width), arrays[0].dtype)
    anywhere = pl.BlockSpec(memory_space=pl.ANY)
    return pl.pallas_call(
        functools.partial(split_kernel, len(arrays), width),
        out_shape=(shape, shape),
        in_specs=[pl.BlockSpec(memory_space=pltpu.HBM)] * len(arrays),
        out_specs=(anywhere, anywhere),
        scratch_shapes=[pltpu.SemaphoreType.DMA((CORES * len(arrays),))],
        compiler_params=pltpu.CompilerParams(vmem_limit_bytes=1 << 20),
        name="split",
    )(*arrays)


def merge_kernel(slots, near, far, *outs):
    core = lax.axis_index("seq") % CORES
    rows = near.shape[1]

    def fill(shards):
        for (begin, col), out in zip(slots, outs):
            end = begin + out.shape[1]
            for shard, source in enumerate(shards):
                low, high = max(begin, shard * rows), min(end, (shard + 1) * rows)
                if low < high:
                    out[:, low - begin : high - begin] = source[
                        :, low - shard * rows : high - shard * rows, col : col + out.shape[2]
                    ]

    pl.when(core == 0)(functools.partial(fill, (near, far)))
    pl.when(core == 1)(functools.partial(fill, (far, near)))


def merge(shapes, near, far):
    near_by = pl.BlockSpec(memory_space=pltpu.VMEM)
    slots = tuple((begin, col) for begin, col, _, _ in shapes)
    return pl.pallas_call(
        functools.partial(merge_kernel, slots),
        out_shape=tuple(
            pltpu.VMEM((near.shape[0], count, width), near.dtype)
            for _, _, count, width in shapes
        ),
        in_specs=[near_by, near_by],
        out_specs=(near_by,) * len(shapes),
        compiler_params=pltpu.CompilerParams(vmem_limit_bytes=12 << 20),
        name="merge",
    )(near, far)


def choose_kernel(own, came, out):
    row = lax.axis_index("seq") // CORES % 2

    @pl.when(row == 0)
    def _():
        out[...] = own[...]

    @pl.when(row == 1)
    def _():
        out[...] = came[...]


def choose(own, came):
    near_by = pl.BlockSpec(memory_space=pltpu.VMEM)
    return pl.pallas_call(
        choose_kernel,
        out_shape=pltpu.VMEM(own.shape, own.dtype),
        in_specs=[near_by, near_by],
        out_specs=near_by,
        compiler_params=pltpu.CompilerParams(vmem_limit_bytes=6 << 20),
        name="choose",
    )(own, came)


def chunk_heads(half):
    sizes = [2] * (half // 2)
    return sizes + [1] * (half % 2)


def on_device(queries, keys, values, doc_blocks):
    devices = lax.axis_size("seq")
    rows = queries.shape[0]
    q_heads = queries.shape[1] // DH
    kv_heads = keys.shape[1] // DH
    ratio = q_heads // kv_heads
    half = kv_heads // CORES
    chips = devices // CORES
    chip_rows = rows * CORES
    window = rows * devices // BLK // 4
    spans = min(-(-(window - 1) * BLK // chip_rows), chips)

    partner = [(i, i ^ 1) for i in range(devices)]
    next_chip = [(i, i + CORES) for i in range(devices - CORES)]
    next_pair = [(i, i + 2 * CORES) for i in range(devices - 2 * CORES)]
    across = [(i, i ^ CORES) for i in range(devices)]

    kv_send, kv_near = split(keys, values)
    kv_far = shift(kv_send, partner)
    q_send, q_near = split(queries)
    q_far = shift(q_send, partner)

    sizes = chunk_heads(half)
    firsts = [sum(sizes[:i]) for i in range(len(sizes))]

    base = spans * chip_rows
    lead = base - (window - 1) * BLK
    paired = spans == 2 and chips % 2 == 0 and 0 < lead <= rows
    width = half * DH
    kept = lead if paired else 0
    shapes = [
        (kept, first * DH, chip_rows - kept, heads * DH) for first, heads in zip(firsts, sizes)
    ]
    leads, lead_near, lead_far = [], [], []
    parts = 2 if paired else 0
    shapes += [(0, part * width // parts, lead, width // parts) for part in range(parts)]
    merged = merge(shapes, kv_near, kv_far)
    own, leads = merged[: len(sizes)], merged[len(sizes) :]
    for part, block in enumerate(leads):
        lead_near.append(shift(block, across))
        lead_far.append(shift(lead_near[part], next_pair))

    nears, fars = [], []
    for i, (first, heads) in enumerate(zip(firsts, sizes)):
        if paired:
            two_back = shift(own[i], next_pair)
            one_back = shift(choose(own[i], two_back), across)
            part = first * DH * parts // width
            col = first * DH - part * width // parts
            pieces = [own[i], one_back, two_back, leads[part], lead_near[part], lead_far[part]]
            spots = (
                (base + lead, 0, None),
                (base - chip_rows + lead, 0, None),
                (base - 2 * chip_rows + lead, 0, None),
                (base, col, None),
                (base - chip_rows, col, 1),
                (base - chip_rows, col, 0),
            )
        else:
            pieces = [own[i]]
            for _ in range(spans):
                pieces.append(shift(pieces[-1], next_chip))
            spots = tuple((base - back * chip_rows, 0, None) for back in range(spans + 1))
        plan = (first, heads, half, ratio, window, spans)
        out_near, out_far = attend(plan, spots, doc_blocks, q_near, q_far, pieces)
        nears.append(out_near)
        fars.append(shift(out_far, partner))
    return place(firsts, half, ratio, nears, fars, queries.shape[1])


def solution(mesh):
    spec = P(("groups", "seq"), None)

    return jax.shard_map(
        on_device,
        mesh=mesh,
        in_specs=(spec, spec, spec, P("groups")),
        out_specs=spec,
        check_vma=False,
    )
```

```python
import functools
import math

import jax
import jax.numpy as jnp
from jax import lax
from jax.experimental import pallas as pl
from jax.experimental.pallas import tpu as pltpu
from jax.sharding import PartitionSpec as P


DH = 128
BLK = 128
CORES = 2
SLOTS = 4
LIMIT = 58 << 20
PART = 16
SCALE = 144.0 ** (-0.5)


def shift(block, pairs):
    return lax.ppermute(block, "seq", pairs)


def attend_kernel(plan, spots, blocks, q_near, q_far, *rest):
    first, heads, _, ratio, window, spans = plan
    pieces = rest[: len(spots)]
    out_near, out_far, q_buf, k_buf, v_buf, o_buf, s_buf, w_buf = rest[len(spots) :]
    rows = q_near.shape[-2]
    chip_rows = rows * CORES
    me = lax.axis_index("seq")
    core = me % CORES
    chip = me // CORES
    q_width = heads * DH * ratio
    base = spans * chip_rows
    q_cols = slice(first * DH * ratio, first * DH * ratio + q_width)
    mine = pl.multiple_of(core * rows, rows)
    other = pl.multiple_of((1 - core) * rows, rows)
    q_buf[pl.ds(mine, rows)] = q_near[0, :, q_cols]
    q_buf[pl.ds(other, rows)] = q_far[0, :, q_cols]

    def bring(piece, at, low, high, col):
        to = slice(at, at + high - low)
        k_buf[to] = piece[0, low:high, col : col + heads * DH]
        v_buf[to] = piece[1, low:high, col : col + heads * DH]

    tests = {"side": chip % 2, "core": core}
    for piece, (at, low, high, col, test) in zip(pieces, spots):
        if test is None:
            bring(piece, at, low, high, col)
        else:
            name, wanted = test
            pl.when(tests[name] == wanted)(
                functools.partial(bring, piece, at, low, high, col)
            )

    units = chip_rows // BLK
    factor = SCALE * math.log2(math.e)
    tile_rows = ratio * BLK
    keys_seen = window * BLK
    last = lax.broadcasted_iota(jnp.int32, (BLK, BLK), 1)
    row = lax.broadcasted_iota(jnp.int32, (BLK, BLK), 0)
    causal = jnp.where(last <= row, 0.0, -1e30)
    key = lax.broadcasted_iota(jnp.int32, (8, keys_seen - BLK), 1)
    ones = jnp.ones((keys_seen, DH), jnp.bfloat16)

    def keys_of(unit):
        first_key = base + (unit + 1 - window) * BLK
        return pl.ds(first_key, keys_seen)

    def score(unit, group):
        q_at = pl.ds(unit * BLK, BLK)
        tiles = [
            q_buf[q_at, (group * ratio + s) * DH : (group * ratio + s + 1) * DH]
            for s in range(ratio)
        ]
        s_buf[(unit * heads + group) % SLOTS] = lax.dot_general(
            jnp.concatenate(tiles, axis=0),
            k_buf[keys_of(unit), group * DH : (group + 1) * DH],
            (((1,), (1,)), ((), ())),
            preferred_element_type=jnp.float32,
        )

    def weigh(unit, group):
        number = chip * units + unit
        begin = jnp.int32(0)
        total = jnp.int32(0)
        for doc in range(blocks.shape[0]):
            begin = jnp.where(number >= total, total, begin)
            total = total + blocks[doc]
        hidden = (window - 1 - number + begin) * BLK
        before = jnp.where(key >= hidden, 0.0, -1e30)
        before = jnp.concatenate([before] * (PART // 8), axis=0)
        slot = (unit * heads + group) % SLOTS
        for part in range(tile_rows // PART):
            at = slice(part * PART, (part + 1) * PART)
            low = part * PART % BLK
            bias = jnp.concatenate([before, causal[low : low + PART]], axis=1)
            scores = s_buf[slot, at] * factor + bias
            top = jnp.max(scores, axis=1, keepdims=True)
            w_buf[slot, at] = jnp.exp2(scores - top).astype(jnp.bfloat16)

    def blend(unit, group):
        v_part = v_buf[keys_of(unit), group * DH : (group + 1) * DH]
        blended = jnp.dot(
            w_buf[(unit * heads + group) % SLOTS],
            jnp.concatenate([v_part, ones], axis=1),
            preferred_element_type=jnp.float32,
        )
        blended = (blended[:, :DH] / blended[:, DH:]).astype(jnp.bfloat16)
        for s in range(ratio):
            cols = slice((group * ratio + s) * DH, (group * ratio + s + 1) * DH)
            o_buf[pl.ds(unit * BLK, BLK), cols] = blended[s * BLK : (s + 1) * BLK]

    tiles = [(unit, group) for unit in range(units) for group in range(heads)]
    for step in range(len(tiles) + 2):
        if step < len(tiles):
            score(*tiles[step])
        if 0 <= step - 1 < len(tiles):
            weigh(*tiles[step - 1])
        if 0 <= step - 2:
            blend(*tiles[step - 2])
    out_near[...] = o_buf[pl.ds(mine, rows)]
    out_far[...] = o_buf[pl.ds(other, rows)]


def attend(plan, spots, blocks, q_near, q_far, pieces):
    _, heads, _, ratio, window, spans = plan
    rows = q_near.shape[-2]
    chip_rows = rows * CORES
    held = (spans + 1) * chip_rows
    kv_width = heads * DH
    q_width = kv_width * ratio
    scores = heads * ratio * chip_rows * window * BLK
    scratch_bytes = (chip_rows * q_width + held * kv_width) * 4 + SLOTS * ratio * BLK * window * BLK * 6
    near_by = pl.BlockSpec(memory_space=pltpu.VMEM)
    shape = pltpu.VMEM((rows, q_width), q_near.dtype)
    return pl.pallas_call(
        functools.partial(attend_kernel, plan, spots),
        out_shape=(shape, shape),
        in_specs=[pl.BlockSpec(memory_space=pltpu.SMEM)] + [near_by] * (2 + len(pieces)),
        out_specs=(near_by, near_by),
        scratch_shapes=[
            pltpu.VMEM((chip_rows, q_width), jnp.bfloat16),
            pltpu.VMEM((held, kv_width), jnp.bfloat16),
            pltpu.VMEM((held, kv_width), jnp.bfloat16),
            pltpu.VMEM((chip_rows, q_width), jnp.bfloat16),
            pltpu.VMEM((SLOTS, ratio * BLK, window * BLK), jnp.float32),
            pltpu.VMEM((SLOTS, ratio * BLK, window * BLK), jnp.bfloat16),
        ],
        cost_estimate=pl.CostEstimate(
            flops=4 * scores * DH,
            bytes_accessed=2 * (chip_rows * q_width * 2 + held * kv_width * 2),
            transcendentals=scores,
        ),
        compiler_params=pltpu.CompilerParams(vmem_limit_bytes=scratch_bytes + (6 << 20)),
    )(blocks, q_near, q_far, *pieces)


def place_kernel(firsts, half, ratio, *refs):
    count = len(firsts)
    out, sems = refs[2 * count :]
    core = lax.axis_index("seq") % CORES
    stores = []
    for i, first in enumerate(firsts):
        for which, piece in ((core, refs[i]), (1 - core, refs[count + i])):
            col = pl.multiple_of((which * half + first) * ratio * DH, DH)
            store = pltpu.make_async_copy(
                piece, out.at[:, pl.ds(col, piece.shape[1])], sems.at[len(stores)]
            )
            store.start()
            stores.append(store)
    for store in stores:
        store.wait()


def place(firsts, half, ratio, nears, fars, width):
    anywhere = pl.BlockSpec(memory_space=pl.ANY)
    return pl.pallas_call(
        functools.partial(place_kernel, firsts, half, ratio),
        out_shape=pltpu.HBM((nears[0].shape[0], width), nears[0].dtype),
        in_specs=[anywhere] * (2 * len(firsts)),
        out_specs=anywhere,
        scratch_shapes=[pltpu.SemaphoreType.DMA((2 * len(firsts),))],
        compiler_params=pltpu.CompilerParams(vmem_limit_bytes=1 << 20),
        name="place",
    )(*nears, *fars)


def split_kernel(arrays, width, early, *refs):
    sources, outs, sems = refs[:arrays], refs[arrays:-1], refs[-1]
    core = lax.axis_index("seq") % CORES
    copies = []
    for out, which, count in zip(
        outs, (1 - core, core, core, 1 - core), (width, width, early, early)
    ):
        for i in range(arrays):
            col = pl.multiple_of(which * width, DH)
            copy = pltpu.make_async_copy(
                sources[i].at[:, pl.ds(col, count)], out.at[i], sems.at[len(copies)]
            )
            copy.start()
            copies.append(copy)
    for copy in copies:
        copy.wait()


def split(early, limit, *arrays):
    rows, columns = arrays[0].shape
    width = columns // CORES
    counts = [width] * 2 + [early] * (2 if early else 0)
    anywhere = pl.BlockSpec(memory_space=pl.ANY)
    return pl.pallas_call(
        functools.partial(split_kernel, len(arrays), width, early),
        out_shape=tuple(
            pltpu.VMEM((len(arrays), rows, count), arrays[0].dtype) for count in counts
        ),
        in_specs=[pl.BlockSpec(memory_space=pltpu.HBM)] * len(arrays),
        out_specs=(anywhere,) * len(counts),
        scratch_shapes=[pltpu.SemaphoreType.DMA((len(counts) * len(arrays),))],
        compiler_params=pltpu.CompilerParams(vmem_limit_bytes=limit),
        name="split",
    )(*arrays)


def merge_kernel(slots, near, far, *outs):
    core = lax.axis_index("seq") % CORES
    rows = near.shape[1]

    def fill(shards):
        for (begin, col), out in zip(slots, outs):
            end = begin + out.shape[1]
            for shard, source in enumerate(shards):
                low, high = max(begin, shard * rows), min(end, (shard + 1) * rows)
                if low < high:
                    out[:, low - begin : high - begin] = source[
                        :, low - shard * rows : high - shard * rows, col : col + out.shape[2]
                    ]

    pl.when(core == 0)(functools.partial(fill, (near, far)))
    pl.when(core == 1)(functools.partial(fill, (far, near)))


def merge(shapes, near, far):
    near_by = pl.BlockSpec(memory_space=pltpu.VMEM)
    slots = tuple((begin, col) for begin, col, _, _ in shapes)
    return pl.pallas_call(
        functools.partial(merge_kernel, slots),
        out_shape=tuple(
            pltpu.VMEM((near.shape[0], count, width), near.dtype)
            for _, _, count, width in shapes
        ),
        in_specs=[near_by, near_by],
        out_specs=(near_by,) * len(shapes),
        compiler_params=pltpu.CompilerParams(vmem_limit_bytes=12 << 20),
        name="merge",
    )(near, far)


def choose_kernel(own, *refs):
    came, out = refs[:-1], refs[-1]
    me = lax.axis_index("seq")
    core = me % CORES
    row = me // CORES % 2

    @pl.when(row == 0)
    def _():
        out[...] = own[...]

    @pl.when(row == 1)
    def _():
        if len(came) == 1:
            out[...] = came[0][...]
        else:
            rows = came[0].shape[1]
            out[:, pl.ds(pl.multiple_of(core * rows, rows), rows)] = came[0][...]
            out[:, pl.ds(pl.multiple_of((1 - core) * rows, rows), rows)] = came[1][...]


def choose(own, *came):
    near_by = pl.BlockSpec(memory_space=pltpu.VMEM)
    return pl.pallas_call(
        choose_kernel,
        out_shape=pltpu.VMEM(own.shape, own.dtype),
        in_specs=[near_by] * (1 + len(came)),
        out_specs=near_by,
        compiler_params=pltpu.CompilerParams(vmem_limit_bytes=6 << 20),
        name="choose",
    )(own, *came)


def chunk_heads(half):
    sizes = []
    while sum(sizes) + 2 < half:
        sizes.append(2)
    return sizes + [1] * (half - sum(sizes))


def on_device(queries, keys, values, doc_blocks):
    devices = lax.axis_size("seq")
    rows = queries.shape[0]
    q_heads = queries.shape[1] // DH
    kv_heads = keys.shape[1] // DH
    ratio = q_heads // kv_heads
    half = kv_heads // CORES
    chips = devices // CORES
    chip_rows = rows * CORES
    window = rows * devices // BLK // 4
    spans = min(-(-(window - 1) * BLK // chip_rows), chips)

    partner = [(i, i ^ 1) for i in range(devices)]
    next_chip = [(i, i + CORES) for i in range(devices - CORES)]
    next_pair = [(i, i + 2 * CORES) for i in range(devices - 2 * CORES)]
    across = [(i, i ^ CORES) for i in range(devices)]

    sizes = chunk_heads(half)
    firsts = [sum(sizes[:i]) for i in range(len(sizes))]
    base = spans * chip_rows
    lead = base - (window - 1) * BLK
    paired = spans == 2 and chips % 2 == 0 and 0 < lead <= rows
    width = half * DH
    crossed = [(i, (i + 2 * CORES) ^ 1) for i in range(devices - 2 * CORES)]
    early = sizes[0] * DH if paired else 0
    kv_send, kv_near, *firstly = split(early, LIMIT, keys, values)
    kv_far = shift(kv_send, partner)
    if paired:
        straight = shift(firstly[0], next_pair)
        cross = shift(firstly[1], crossed)
    q_send, q_near = split(0, 1 << 20, queries)
    q_far = shift(q_send, partner)

    shapes = []
    for i, (first, heads) in enumerate(zip(firsts, sizes)):
        low = lead if paired and i > 0 else 0
        shapes.append((low, first * DH, chip_rows - low, heads * DH))
    if paired:
        shapes.append((0, early, lead, width - early))
    merged = merge(shapes, kv_near, kv_far)
    own = merged[: len(sizes)]
    if paired:
        lead_near = shift(merged[-1], across)
        lead_far = shift(lead_near, next_pair)

    nears, fars = [], []
    for i, (first, heads) in enumerate(zip(firsts, sizes)):
        if paired:
            if i == 0:
                two_back = (straight, cross)
            else:
                two_back = (shift(own[i], next_pair),)
            chosen = choose(own[i], *two_back)
            one_back = shift(chosen, across)
            low = shapes[i][0]
            count = chip_rows - low
            one, two = base - chip_rows, base - 2 * chip_rows
            pieces = [own[i], one_back]
            spots = ((base + low, 0, count, 0, None), (one + low, 0, count, 0, None))
            if i == 0:
                for core, (same, other) in enumerate(((two, two + rows), (two + rows, two))):
                    pieces += [straight, cross]
                    spots += (
                        (same, 0, rows, 0, ("core", core)),
                        (other, 0, rows, 0, ("core", core)),
                    )
            else:
                pieces += [*two_back, merged[-1], lead_near, lead_far]
                col = first * DH - early
                spots += (
                    (two + low, 0, count, 0, None),
                    (base, 0, lead, col, None),
                    (one, 0, lead, col, ("side", 1)),
                    (one, 0, lead, col, ("side", 0)),
                )
        else:
            pieces = [own[i]]
            for _ in range(spans):
                pieces.append(shift(pieces[-1], next_chip))
            spots = tuple(
                (base - back * chip_rows, 0, chip_rows, 0, None) for back in range(spans + 1)
            )
        plan = (first, heads, half, ratio, window, spans)
        out_near, out_far = attend(plan, spots, doc_blocks, q_near, q_far, pieces)
        nears.append(out_near)
        fars.append(shift(out_far, partner))
    return place(firsts, half, ratio, nears, fars, queries.shape[1])


def solution(mesh):
    spec = P(("groups", "seq"), None)

    return jax.shard_map(
        on_device,
        mesh=mesh,
        in_specs=(spec, spec, spec, P("groups")),
        out_specs=spec,
        check_vma=False,
    )
```

```python
import functools
import math

import jax
import jax.numpy as jnp
from jax import lax
from jax.experimental import pallas as pl
from jax.experimental.pallas import tpu as pltpu
from jax.sharding import PartitionSpec as P


DH = 128
BLK = 128
CORES = 2
SLOTS = 4
LIMIT = 58 << 20
PART = 16
SCALE = 144.0 ** (-0.5)


def shift(block, pairs):
    return lax.ppermute(block, "seq", pairs)


def attend_kernel(plan, spots, blocks, q_near, q_far, *rest):
    first, heads, _, ratio, window, spans = plan
    pieces = rest[: len(spots)]
    out_near, out_far, q_buf, k_buf, v_buf, o_buf, s_buf, w_buf = rest[len(spots) :]
    rows = q_near.shape[-2]
    chip_rows = rows * CORES
    me = lax.axis_index("seq")
    core = me % CORES
    chip = me // CORES
    q_width = heads * DH * ratio
    base = spans * chip_rows
    q_cols = slice(first * DH * ratio, first * DH * ratio + q_width)
    mine = pl.multiple_of(core * rows, rows)
    other = pl.multiple_of((1 - core) * rows, rows)
    q_buf[pl.ds(mine, rows)] = q_near[0, :, q_cols]
    q_buf[pl.ds(other, rows)] = q_far[0, :, q_cols]

    def bring(piece, at, low, high, col):
        to = slice(at, at + high - low)
        k_buf[to] = piece[0, low:high, col : col + heads * DH]
        v_buf[to] = piece[1, low:high, col : col + heads * DH]

    tests = {"side": chip % 2, "core": core}
    for piece, (at, low, high, col, test) in zip(pieces, spots):
        if test is None:
            bring(piece, at, low, high, col)
        else:
            name, wanted = test
            pl.when(tests[name] == wanted)(
                functools.partial(bring, piece, at, low, high, col)
            )

    units = chip_rows // BLK
    factor = SCALE * math.log2(math.e)
    tile_rows = ratio * BLK
    keys_seen = window * BLK
    last = lax.broadcasted_iota(jnp.int32, (BLK, BLK), 1)
    row = lax.broadcasted_iota(jnp.int32, (BLK, BLK), 0)
    causal = jnp.where(last <= row, 0.0, -1e30)
    key = lax.broadcasted_iota(jnp.int32, (8, keys_seen - BLK), 1)
    ones = jnp.ones((keys_seen, DH), jnp.bfloat16)

    def keys_of(unit):
        first_key = base + (unit + 1 - window) * BLK
        return pl.ds(first_key, keys_seen)

    def score(unit, group):
        q_at = pl.ds(unit * BLK, BLK)
        tiles = [
            q_buf[q_at, (group * ratio + s) * DH : (group * ratio + s + 1) * DH]
            for s in range(ratio)
        ]
        s_buf[(unit * heads + group) % SLOTS] = lax.dot_general(
            jnp.concatenate(tiles, axis=0),
            k_buf[keys_of(unit), group * DH : (group + 1) * DH],
            (((1,), (1,)), ((), ())),
            preferred_element_type=jnp.float32,
        )

    def weigh(unit, group):
        number = chip * units + unit
        begin = jnp.int32(0)
        total = jnp.int32(0)
        for doc in range(blocks.shape[0]):
            begin = jnp.where(number >= total, total, begin)
            total = total + blocks[doc]
        hidden = (window - 1 - number + begin) * BLK
        before = jnp.where(key >= hidden, 0.0, -1e30)
        before = jnp.concatenate([before] * (PART // 8), axis=0)
        slot = (unit * heads + group) % SLOTS
        for part in range(tile_rows // PART):
            at = slice(part * PART, (part + 1) * PART)
            low = part * PART % BLK
            bias = jnp.concatenate([before, causal[low : low + PART]], axis=1)
            scores = s_buf[slot, at] * factor + bias
            top = jnp.max(scores, axis=1, keepdims=True)
            w_buf[slot, at] = jnp.exp2(scores - top).astype(jnp.bfloat16)

    def blend(unit, group):
        v_part = v_buf[keys_of(unit), group * DH : (group + 1) * DH]
        blended = jnp.dot(
            w_buf[(unit * heads + group) % SLOTS],
            jnp.concatenate([v_part, ones], axis=1),
            preferred_element_type=jnp.float32,
        )
        blended = (blended[:, :DH] / blended[:, DH:]).astype(jnp.bfloat16)
        for s in range(ratio):
            cols = slice((group * ratio + s) * DH, (group * ratio + s + 1) * DH)
            o_buf[pl.ds(unit * BLK, BLK), cols] = blended[s * BLK : (s + 1) * BLK]

    tiles = [(unit, group) for unit in range(units) for group in range(heads)]
    for step in range(len(tiles) + 2):
        if step < len(tiles):
            score(*tiles[step])
        if 0 <= step - 1 < len(tiles):
            weigh(*tiles[step - 1])
        if 0 <= step - 2:
            blend(*tiles[step - 2])
    out_near[...] = o_buf[pl.ds(mine, rows)]
    out_far[...] = o_buf[pl.ds(other, rows)]


def attend(plan, spots, blocks, q_near, q_far, pieces):
    _, heads, _, ratio, window, spans = plan
    rows = q_near.shape[-2]
    chip_rows = rows * CORES
    held = (spans + 1) * chip_rows
    kv_width = heads * DH
    q_width = kv_width * ratio
    scores = heads * ratio * chip_rows * window * BLK
    scratch_bytes = (chip_rows * q_width + held * kv_width) * 4 + SLOTS * ratio * BLK * window * BLK * 6
    near_by = pl.BlockSpec(memory_space=pltpu.VMEM)
    shape = pltpu.VMEM((rows, q_width), q_near.dtype)
    return pl.pallas_call(
        functools.partial(attend_kernel, plan, spots),
        out_shape=(shape, shape),
        in_specs=[pl.BlockSpec(memory_space=pltpu.SMEM)] + [near_by] * (2 + len(pieces)),
        out_specs=(near_by, near_by),
        scratch_shapes=[
            pltpu.VMEM((chip_rows, q_width), jnp.bfloat16),
            pltpu.VMEM((held, kv_width), jnp.bfloat16),
            pltpu.VMEM((held, kv_width), jnp.bfloat16),
            pltpu.VMEM((chip_rows, q_width), jnp.bfloat16),
            pltpu.VMEM((SLOTS, ratio * BLK, window * BLK), jnp.float32),
            pltpu.VMEM((SLOTS, ratio * BLK, window * BLK), jnp.bfloat16),
        ],
        cost_estimate=pl.CostEstimate(
            flops=4 * scores * DH,
            bytes_accessed=2 * (chip_rows * q_width * 2 + held * kv_width * 2),
            transcendentals=scores,
        ),
        compiler_params=pltpu.CompilerParams(vmem_limit_bytes=scratch_bytes + (6 << 20)),
    )(blocks, q_near, q_far, *pieces)


def place_kernel(firsts, half, ratio, *refs):
    count = len(firsts)
    out, sems = refs[2 * count :]
    core = lax.axis_index("seq") % CORES
    stores = []
    for i, first in enumerate(firsts):
        for which, piece in ((core, refs[i]), (1 - core, refs[count + i])):
            col = pl.multiple_of((which * half + first) * ratio * DH, DH)
            store = pltpu.make_async_copy(
                piece, out.at[:, pl.ds(col, piece.shape[1])], sems.at[len(stores)]
            )
            store.start()
            stores.append(store)
    for store in stores:
        store.wait()


def place(firsts, half, ratio, nears, fars, width):
    anywhere = pl.BlockSpec(memory_space=pl.ANY)
    return pl.pallas_call(
        functools.partial(place_kernel, firsts, half, ratio),
        out_shape=pltpu.HBM((nears[0].shape[0], width), nears[0].dtype),
        in_specs=[anywhere] * (2 * len(firsts)),
        out_specs=anywhere,
        scratch_shapes=[pltpu.SemaphoreType.DMA((2 * len(firsts),))],
        compiler_params=pltpu.CompilerParams(vmem_limit_bytes=1 << 20),
        name="place",
    )(*nears, *fars)


def split_kernel(arrays, width, early, *refs):
    sources, outs, sems = refs[:arrays], refs[arrays:-1], refs[-1]
    core = lax.axis_index("seq") % CORES
    copies = []
    for out, which, count in zip(
        outs, (1 - core, core, core, 1 - core), (width, width, early, early)
    ):
        for i in range(arrays):
            col = pl.multiple_of(which * width, DH)
            copy = pltpu.make_async_copy(
                sources[i].at[:, pl.ds(col, count)], out.at[i], sems.at[len(copies)]
            )
            copy.start()
            copies.append(copy)
    for copy in copies:
        copy.wait()


def split(early, limit, *arrays):
    rows, columns = arrays[0].shape
    width = columns // CORES
    counts = [width] * 2 + [early] * (2 if early else 0)
    anywhere = pl.BlockSpec(memory_space=pl.ANY)
    return pl.pallas_call(
        functools.partial(split_kernel, len(arrays), width, early),
        out_shape=tuple(
            pltpu.VMEM((len(arrays), rows, count), arrays[0].dtype) for count in counts
        ),
        in_specs=[pl.BlockSpec(memory_space=pltpu.HBM)] * len(arrays),
        out_specs=(anywhere,) * len(counts),
        scratch_shapes=[pltpu.SemaphoreType.DMA((len(counts) * len(arrays),))],
        compiler_params=pltpu.CompilerParams(vmem_limit_bytes=limit),
        name="split",
    )(*arrays)


def merge_kernel(slots, near, far, *outs):
    core = lax.axis_index("seq") % CORES
    rows = near.shape[1]

    def fill(shards):
        for (begin, col), out in zip(slots, outs):
            end = begin + out.shape[1]
            for shard, source in enumerate(shards):
                low, high = max(begin, shard * rows), min(end, (shard + 1) * rows)
                if low < high:
                    out[:, low - begin : high - begin] = source[
                        :, low - shard * rows : high - shard * rows, col : col + out.shape[2]
                    ]

    pl.when(core == 0)(functools.partial(fill, (near, far)))
    pl.when(core == 1)(functools.partial(fill, (far, near)))


def merge(shapes, near, far):
    near_by = pl.BlockSpec(memory_space=pltpu.VMEM)
    slots = tuple((begin, col) for begin, col, _, _ in shapes)
    return pl.pallas_call(
        functools.partial(merge_kernel, slots),
        out_shape=tuple(
            pltpu.VMEM((near.shape[0], count, width), near.dtype)
            for _, _, count, width in shapes
        ),
        in_specs=[near_by, near_by],
        out_specs=(near_by,) * len(shapes),
        compiler_params=pltpu.CompilerParams(vmem_limit_bytes=12 << 20),
        name="merge",
    )(near, far)


def choose_kernel(own, *refs):
    came, out = refs[:-1], refs[-1]
    me = lax.axis_index("seq")
    core = me % CORES
    row = me // CORES % 2

    @pl.when(row == 0)
    def _():
        out[...] = own[...]

    @pl.when(row == 1)
    def _():
        if len(came) == 1:
            out[...] = came[0][...]
        else:
            rows = came[0].shape[1]
            out[:, pl.ds(pl.multiple_of(core * rows, rows), rows)] = came[0][...]
            out[:, pl.ds(pl.multiple_of((1 - core) * rows, rows), rows)] = came[1][...]


def choose(own, *came):
    near_by = pl.BlockSpec(memory_space=pltpu.VMEM)
    return pl.pallas_call(
        choose_kernel,
        out_shape=pltpu.VMEM(own.shape, own.dtype),
        in_specs=[near_by] * (1 + len(came)),
        out_specs=near_by,
        compiler_params=pltpu.CompilerParams(vmem_limit_bytes=6 << 20),
        name="choose",
    )(own, *came)


def chunk_heads(half):
    if half < 4:
        return [1] * half
    return [1] + [2] * ((half - 2) // 2) + [1] * (half % 2 + 1)


def on_device(queries, keys, values, doc_blocks):
    devices = lax.axis_size("seq")
    rows = queries.shape[0]
    q_heads = queries.shape[1] // DH
    kv_heads = keys.shape[1] // DH
    ratio = q_heads // kv_heads
    half = kv_heads // CORES
    chips = devices // CORES
    chip_rows = rows * CORES
    window = rows * devices // BLK // 4
    spans = min(-(-(window - 1) * BLK // chip_rows), chips)

    partner = [(i, i ^ 1) for i in range(devices)]
    next_chip = [(i, i + CORES) for i in range(devices - CORES)]
    next_pair = [(i, (i + 2 * CORES) % devices) for i in range(devices)]
    across = [(i, i ^ CORES) for i in range(devices)]

    sizes = chunk_heads(half)
    firsts = [sum(sizes[:i]) for i in range(len(sizes))]
    base = spans * chip_rows
    lead = base - (window - 1) * BLK
    paired = spans == 2 and chips % 2 == 0 and 0 < lead <= rows
    crossed = [(i, (i + 2 * CORES) % devices ^ 1) for i in range(devices)]
    early = sizes[0] * DH if paired else 0
    kv_send, kv_near, *firstly = split(early, LIMIT, keys, values)
    kv_far = shift(kv_send, partner)
    if paired:
        straight = shift(firstly[0], next_pair)
        cross = shift(firstly[1], crossed)
    q_send, q_near = split(0, 1 << 20, queries)
    q_far = shift(q_send, partner)

    shapes = []
    for i, (first, heads) in enumerate(zip(firsts, sizes)):
        low = lead if paired and i > 0 else 0
        shapes.append((low, first * DH, chip_rows - low, heads * DH))
    groups = ()
    if paired:
        middle = 1 + len(sizes) // 2
        ends = (firsts[1], firsts[middle], half)
        groups = tuple(zip(ends, ends[1:]))
        shapes += [(0, low * DH, lead, (high - low) * DH) for low, high in groups]
    merged = merge(shapes, kv_near, kv_far)
    own = merged[: len(sizes)]
    leads, leads_near, leads_far = merged[len(sizes) :], [], []
    for g, block in enumerate(leads):
        leads_near.append(shift(block, across))
        leads_far.append(shift(leads_near[g], next_pair))

    nears, fars = [], []
    for i, (first, heads) in enumerate(zip(firsts, sizes)):
        if paired:
            if i == 0:
                two_back = (straight, cross)
            else:
                two_back = (shift(own[i], next_pair),)
            chosen = choose(own[i], *two_back)
            one_back = shift(chosen, across)
            low = shapes[i][0]
            count = chip_rows - low
            one, two = base - chip_rows, base - 2 * chip_rows
            pieces = [own[i], one_back]
            spots = ((base + low, 0, count, 0, None), (one + low, 0, count, 0, None))
            if i == 0:
                for core, (same, other) in enumerate(((two, two + rows), (two + rows, two))):
                    pieces += [straight, cross]
                    spots += (
                        (same, 0, rows, 0, ("core", core)),
                        (other, 0, rows, 0, ("core", core)),
                    )
            else:
                g = 0 if i < middle else 1
                pieces += [*two_back, leads[g], leads_near[g], leads_far[g]]
                col = (first - groups[g][0]) * DH
                spots += (
                    (two + low, 0, count, 0, None),
                    (base, 0, lead, col, None),
                    (one, 0, lead, col, ("side", 1)),
                    (one, 0, lead, col, ("side", 0)),
                )
        else:
            pieces = [own[i]]
            for _ in range(spans):
                pieces.append(shift(pieces[-1], next_chip))
            spots = tuple(
                (base - back * chip_rows, 0, chip_rows, 0, None) for back in range(spans + 1)
            )
        plan = (first, heads, half, ratio, window, spans)
        out_near, out_far = attend(plan, spots, doc_blocks, q_near, q_far, pieces)
        nears.append(out_near)
        fars.append(shift(out_far, partner))
    return place(firsts, half, ratio, nears, fars, queries.shape[1])


def solution(mesh):
    spec = P(("groups", "seq"), None)

    return jax.shard_map(
        on_device,
        mesh=mesh,
        in_specs=(spec, spec, spec, P("groups")),
        out_specs=spec,
        check_vma=False,
    )
```

```python
import functools
import math

import jax
import jax.numpy as jnp
from jax import lax
from jax.experimental import pallas as pl
from jax.experimental.pallas import tpu as pltpu
from jax.sharding import PartitionSpec as P


DH = 128
BLK = 128
CORES = 2
SLOTS = 4
WHOLE = 2
LIMIT = 58 << 20
PART = 16
SCALE = 144.0 ** (-0.5)


def shift(block, pairs):
    return lax.ppermute(block, "seq", pairs)


def attend_kernel(plan, spots, blocks, q_near, q_far, *rest):
    first, heads, _, ratio, window, spans = plan
    pieces = rest[: len(spots)]
    out_near, out_far, q_buf, k_buf, v_buf, o_buf, s_buf, w_buf = rest[len(spots) :]
    rows = q_near.shape[-2]
    chip_rows = rows * CORES
    me = lax.axis_index("seq")
    core = me % CORES
    chip = me // CORES
    q_width = heads * DH * ratio
    base = spans * chip_rows
    q_cols = slice(first * DH * ratio, first * DH * ratio + q_width)
    mine = pl.multiple_of(core * rows, rows)
    other = pl.multiple_of((1 - core) * rows, rows)
    q_buf[pl.ds(mine, rows)] = q_near[0, :, q_cols]
    q_buf[pl.ds(other, rows)] = q_far[0, :, q_cols]

    def bring(piece, at, low, high, col):
        to = slice(at, at + high - low)
        k_buf[to] = piece[0, low:high, col : col + heads * DH]
        v_buf[to] = piece[1, low:high, col : col + heads * DH]

    tests = {"side": chip % 2, "core": core}
    for piece, (at, low, high, col, test) in zip(pieces, spots):
        if test is None:
            bring(piece, at, low, high, col)
        else:
            name, wanted = test
            pl.when(tests[name] == wanted)(
                functools.partial(bring, piece, at, low, high, col)
            )

    units = chip_rows // BLK
    factor = SCALE * math.log2(math.e)
    tile_rows = ratio * BLK
    keys_seen = window * BLK
    last = lax.broadcasted_iota(jnp.int32, (BLK, BLK), 1)
    row = lax.broadcasted_iota(jnp.int32, (BLK, BLK), 0)
    causal = jnp.where(last <= row, 0.0, -1e30)
    key = lax.broadcasted_iota(jnp.int32, (8, keys_seen - BLK), 1)
    ones = jnp.ones((keys_seen, DH), jnp.bfloat16)

    def keys_of(unit):
        first_key = base + (unit + 1 - window) * BLK
        return pl.ds(first_key, keys_seen)

    def score(unit, group):
        q_at = pl.ds(unit * BLK, BLK)
        tiles = [
            q_buf[q_at, (group * ratio + s) * DH : (group * ratio + s + 1) * DH]
            for s in range(ratio)
        ]
        s_buf[(unit * heads + group) % SLOTS] = lax.dot_general(
            jnp.concatenate(tiles, axis=0),
            k_buf[keys_of(unit), group * DH : (group + 1) * DH],
            (((1,), (1,)), ((), ())),
            preferred_element_type=jnp.float32,
        )

    def weigh(unit, group):
        number = chip * units + unit
        begin = jnp.int32(0)
        total = jnp.int32(0)
        for doc in range(blocks.shape[0]):
            begin = jnp.where(number >= total, total, begin)
            total = total + blocks[doc]
        hidden = (window - 1 - number + begin) * BLK
        before = jnp.where(key >= hidden, 0.0, -1e30)
        before = jnp.concatenate([before] * (PART // 8), axis=0)
        slot = (unit * heads + group) % SLOTS
        for part in range(tile_rows // PART):
            at = slice(part * PART, (part + 1) * PART)
            low = part * PART % BLK
            bias = jnp.concatenate([before, causal[low : low + PART]], axis=1)
            scores = s_buf[slot, at] * factor + bias
            top = jnp.max(scores, axis=1, keepdims=True)
            w_buf[slot, at] = jnp.exp2(scores - top).astype(jnp.bfloat16)

    def blend(unit, group):
        v_part = v_buf[keys_of(unit), group * DH : (group + 1) * DH]
        blended = jnp.dot(
            w_buf[(unit * heads + group) % SLOTS],
            jnp.concatenate([v_part, ones], axis=1),
            preferred_element_type=jnp.float32,
        )
        blended = (blended[:, :DH] / blended[:, DH:]).astype(jnp.bfloat16)
        for s in range(ratio):
            cols = slice((group * ratio + s) * DH, (group * ratio + s + 1) * DH)
            o_buf[pl.ds(unit * BLK, BLK), cols] = blended[s * BLK : (s + 1) * BLK]

    tiles = [(unit, group) for unit in range(units) for group in range(heads)]
    for step in range(len(tiles) + 2):
        if step < len(tiles):
            score(*tiles[step])
        if 0 <= step - 1 < len(tiles):
            weigh(*tiles[step - 1])
        if 0 <= step - 2:
            blend(*tiles[step - 2])
    out_near[...] = o_buf[pl.ds(mine, rows)]
    out_far[...] = o_buf[pl.ds(other, rows)]


def attend(plan, spots, blocks, q_near, q_far, pieces):
    _, heads, _, ratio, window, spans = plan
    rows = q_near.shape[-2]
    chip_rows = rows * CORES
    held = (spans + 1) * chip_rows
    kv_width = heads * DH
    q_width = kv_width * ratio
    scores = heads * ratio * chip_rows * window * BLK
    scratch_bytes = (chip_rows * q_width + held * kv_width) * 4 + SLOTS * ratio * BLK * window * BLK * 6
    near_by = pl.BlockSpec(memory_space=pltpu.VMEM)
    shape = pltpu.VMEM((rows, q_width), q_near.dtype)
    return pl.pallas_call(
        functools.partial(attend_kernel, plan, spots),
        out_shape=(shape, shape),
        in_specs=[pl.BlockSpec(memory_space=pltpu.SMEM)] + [near_by] * (2 + len(pieces)),
        out_specs=(near_by, near_by),
        scratch_shapes=[
            pltpu.VMEM((chip_rows, q_width), jnp.bfloat16),
            pltpu.VMEM((held, kv_width), jnp.bfloat16),
            pltpu.VMEM((held, kv_width), jnp.bfloat16),
            pltpu.VMEM((chip_rows, q_width), jnp.bfloat16),
            pltpu.VMEM((SLOTS, ratio * BLK, window * BLK), jnp.float32),
            pltpu.VMEM((SLOTS, ratio * BLK, window * BLK), jnp.bfloat16),
        ],
        cost_estimate=pl.CostEstimate(
            flops=4 * scores * DH,
            bytes_accessed=2 * (chip_rows * q_width * 2 + held * kv_width * 2),
            transcendentals=scores,
        ),
        compiler_params=pltpu.CompilerParams(vmem_limit_bytes=scratch_bytes + (6 << 20)),
    )(blocks, q_near, q_far, *pieces)


def place_kernel(firsts, half, ratio, *refs):
    count = len(firsts)
    out, sems = refs[2 * count :]
    core = lax.axis_index("seq") % CORES
    stores = []
    for i, first in enumerate(firsts):
        for which, piece in ((core, refs[i]), (1 - core, refs[count + i])):
            col = pl.multiple_of((which * half + first) * ratio * DH, DH)
            store = pltpu.make_async_copy(
                piece, out.at[:, pl.ds(col, piece.shape[1])], sems.at[len(stores)]
            )
            store.start()
            stores.append(store)
    for store in stores:
        store.wait()


def place(firsts, half, ratio, nears, fars, width):
    anywhere = pl.BlockSpec(memory_space=pl.ANY)
    return pl.pallas_call(
        functools.partial(place_kernel, firsts, half, ratio),
        out_shape=pltpu.HBM((nears[0].shape[0], width), nears[0].dtype),
        in_specs=[anywhere] * (2 * len(firsts)),
        out_specs=anywhere,
        scratch_shapes=[pltpu.SemaphoreType.DMA((2 * len(firsts),))],
        compiler_params=pltpu.CompilerParams(vmem_limit_bytes=1 << 20),
        name="place",
    )(*nears, *fars)


def split_kernel(arrays, width, early, *refs):
    sources, outs, sems = refs[:arrays], refs[arrays:-1], refs[-1]
    core = lax.axis_index("seq") % CORES
    copies = []
    for out, which, count in zip(
        outs, (1 - core, core, core, 1 - core), (width, width, early, early)
    ):
        for i in range(arrays):
            col = pl.multiple_of(which * width, DH)
            copy = pltpu.make_async_copy(
                sources[i].at[:, pl.ds(col, count)], out.at[i], sems.at[len(copies)]
            )
            copy.start()
            copies.append(copy)
    for copy in copies:
        copy.wait()


def split(early, limit, *arrays):
    rows, columns = arrays[0].shape
    width = columns // CORES
    counts = [width] * 2 + [early] * (2 if early else 0)
    anywhere = pl.BlockSpec(memory_space=pl.ANY)
    return pl.pallas_call(
        functools.partial(split_kernel, len(arrays), width, early),
        out_shape=tuple(
            pltpu.VMEM((len(arrays), rows, count), arrays[0].dtype) for count in counts
        ),
        in_specs=[pl.BlockSpec(memory_space=pltpu.HBM)] * len(arrays),
        out_specs=(anywhere,) * len(counts),
        scratch_shapes=[pltpu.SemaphoreType.DMA((len(counts) * len(arrays),))],
        compiler_params=pltpu.CompilerParams(vmem_limit_bytes=limit),
        name="split",
    )(*arrays)


def merge_kernel(slots, near, far, *outs):
    core = lax.axis_index("seq") % CORES
    rows = near.shape[1]

    def fill(shards):
        for (begin, col), out in zip(slots, outs):
            end = begin + out.shape[1]
            for shard, source in enumerate(shards):
                low, high = max(begin, shard * rows), min(end, (shard + 1) * rows)
                if low < high:
                    out[:, low - begin : high - begin] = source[
                        :, low - shard * rows : high - shard * rows, col : col + out.shape[2]
                    ]

    pl.when(core == 0)(functools.partial(fill, (near, far)))
    pl.when(core == 1)(functools.partial(fill, (far, near)))


def merge(shapes, near, far):
    near_by = pl.BlockSpec(memory_space=pltpu.VMEM)
    slots = tuple((begin, col) for begin, col, _, _ in shapes)
    return pl.pallas_call(
        functools.partial(merge_kernel, slots),
        out_shape=tuple(
            pltpu.VMEM((near.shape[0], count, width), near.dtype)
            for _, _, count, width in shapes
        ),
        in_specs=[near_by, near_by],
        out_specs=(near_by,) * len(shapes),
        compiler_params=pltpu.CompilerParams(vmem_limit_bytes=12 << 20),
        name="merge",
    )(near, far)


def choose_kernel(own, *refs):
    came, out = refs[:-1], refs[-1]
    me = lax.axis_index("seq")
    core = me % CORES
    row = me // CORES % 2

    @pl.when(row == 0)
    def _():
        out[...] = own[...]

    @pl.when(row == 1)
    def _():
        if len(came) == 1:
            out[...] = came[0][...]
        else:
            rows = came[0].shape[1]
            out[:, pl.ds(pl.multiple_of(core * rows, rows), rows)] = came[0][...]
            out[:, pl.ds(pl.multiple_of((1 - core) * rows, rows), rows)] = came[1][...]


def choose(own, *came):
    near_by = pl.BlockSpec(memory_space=pltpu.VMEM)
    return pl.pallas_call(
        choose_kernel,
        out_shape=pltpu.VMEM(own.shape, own.dtype),
        in_specs=[near_by] * (1 + len(came)),
        out_specs=near_by,
        compiler_params=pltpu.CompilerParams(vmem_limit_bytes=6 << 20),
        name="choose",
    )(own, *came)


def chunk_heads(half):
    if half < 6:
        return [1] * half
    return [1, 1] + [2] * ((half - 4) // 2) + [1] * (half % 2 + 2)


def on_device(queries, keys, values, doc_blocks):
    devices = lax.axis_size("seq")
    rows = queries.shape[0]
    q_heads = queries.shape[1] // DH
    kv_heads = keys.shape[1] // DH
    ratio = q_heads // kv_heads
    half = kv_heads // CORES
    chips = devices // CORES
    chip_rows = rows * CORES
    window = rows * devices // BLK // 4
    spans = min(-(-(window - 1) * BLK // chip_rows), chips)

    partner = [(i, i ^ 1) for i in range(devices)]
    next_chip = [(i, i + CORES) for i in range(devices - CORES)]
    next_pair = [(i, (i + 2 * CORES) % devices) for i in range(devices)]
    across = [(i, i ^ CORES) for i in range(devices)]

    sizes = chunk_heads(half)
    firsts = [sum(sizes[:i]) for i in range(len(sizes))]
    base = spans * chip_rows
    lead = base - (window - 1) * BLK
    paired = spans == 2 and chips % 2 == 0 and 0 < lead <= rows and len(sizes) > WHOLE + 1
    crossed = [(i, (i + 2 * CORES) % devices ^ 1) for i in range(devices)]
    early = sizes[0] * DH if paired else 0
    kv_send, kv_near, *firstly = split(early, LIMIT, keys, values)
    kv_far = shift(kv_send, partner)
    if paired:
        straight = shift(firstly[0], next_pair)
        cross = shift(firstly[1], crossed)
    q_send, q_near = split(0, 1 << 20, queries)
    q_far = shift(q_send, partner)

    shapes = []
    for i, (first, heads) in enumerate(zip(firsts, sizes)):
        low = lead if paired and i >= WHOLE else 0
        shapes.append((low, first * DH, chip_rows - low, heads * DH))
    groups = ()
    if paired:
        middle = len(sizes) // 2 + 1
        ends = (firsts[WHOLE], firsts[middle], half)
        groups = tuple(zip(ends, ends[1:]))
        shapes += [(0, low * DH, lead, (high - low) * DH) for low, high in groups]
    merged = merge(shapes, kv_near, kv_far)
    own = merged[: len(sizes)]
    leads, leads_near, leads_far = merged[len(sizes) :], [], []
    for g, block in enumerate(leads):
        leads_near.append(shift(block, across))
        leads_far.append(shift(leads_near[g], next_pair))

    nears, fars = [], []
    for i, (first, heads) in enumerate(zip(firsts, sizes)):
        if paired:
            if i == 0:
                two_back = (straight, cross)
            else:
                two_back = (shift(own[i], next_pair),)
            chosen = choose(own[i], *two_back)
            one_back = shift(chosen, across)
            low = shapes[i][0]
            count = chip_rows - low
            one, two = base - chip_rows, base - 2 * chip_rows
            pieces = [own[i], one_back]
            spots = ((base + low, 0, count, 0, None), (one + low, 0, count, 0, None))
            if i == 0:
                for core, (same, other) in enumerate(((two, two + rows), (two + rows, two))):
                    pieces += [straight, cross]
                    spots += (
                        (same, 0, rows, 0, ("core", core)),
                        (other, 0, rows, 0, ("core", core)),
                    )
            else:
                pieces += [*two_back]
                spots += ((two + low, 0, count, 0, None),)
            if i >= WHOLE:
                g = 0 if i < middle else 1
                pieces += [leads[g], leads_near[g], leads_far[g]]
                col = (first - groups[g][0]) * DH
                spots += (
                    (base, 0, lead, col, None),
                    (one, 0, lead, col, ("side", 1)),
                    (one, 0, lead, col, ("side", 0)),
                )
        else:
            pieces = [own[i]]
            for _ in range(spans):
                pieces.append(shift(pieces[-1], next_chip))
            spots = tuple(
                (base - back * chip_rows, 0, chip_rows, 0, None) for back in range(spans + 1)
            )
        plan = (first, heads, half, ratio, window, spans)
        out_near, out_far = attend(plan, spots, doc_blocks, q_near, q_far, pieces)
        nears.append(out_near)
        fars.append(shift(out_far, partner))
    return place(firsts, half, ratio, nears, fars, queries.shape[1])


def solution(mesh):
    spec = P(("groups", "seq"), None)

    return jax.shard_map(
        on_device,
        mesh=mesh,
        in_specs=(spec, spec, spec, P("groups")),
        out_specs=spec,
        check_vma=False,
    )
```

```python
import functools
import math

import jax
import jax.numpy as jnp
from jax import lax
from jax.experimental import pallas as pl
from jax.experimental.pallas import tpu as pltpu
from jax.sharding import PartitionSpec as P


DH = 128
BLK = 128
CORES = 2
SLOTS = 4
WHOLE = 2
LIMIT = 58 << 20
PART = 16
SCALE = 144.0 ** (-0.5)


def shift(block, pairs):
    return lax.ppermute(block, "seq", pairs)


def store_pieces(puts, pieces, out, half, ratio, sems):
    core = lax.axis_index("seq") % CORES
    stores = []
    for (swapped, first), piece in zip(puts, pieces):
        which = 1 - core if swapped else core
        col = pl.multiple_of((which * half + first) * ratio * DH, DH)
        store = pltpu.make_async_copy(
            piece, out.at[:, pl.ds(col, piece.shape[1])], sems.at[len(stores)]
        )
        store.start()
        stores.append(store)
    return stores


def attend_kernel(plan, spots, puts, blocks, q_near, q_far, *rest):
    first, heads, half, ratio, window, spans = plan
    pieces = rest[: len(spots)]
    rest = rest[len(spots) :]
    stores = []
    if puts:
        placed, rest = rest[: len(puts)], rest[len(puts) :]
        out, sems = rest[2], rest[-1]
        rest = rest[:2] + rest[3:-1]
        stores = store_pieces(puts, placed, out, half, ratio, sems)
    out_near, out_far, q_buf, k_buf, v_buf, o_buf, s_buf, w_buf = rest
    rows = q_near.shape[-2]
    chip_rows = rows * CORES
    me = lax.axis_index("seq")
    core = me % CORES
    chip = me // CORES
    q_width = heads * DH * ratio
    base = spans * chip_rows
    q_cols = slice(first * DH * ratio, first * DH * ratio + q_width)
    mine = pl.multiple_of(core * rows, rows)
    other = pl.multiple_of((1 - core) * rows, rows)
    q_buf[pl.ds(mine, rows)] = q_near[0, :, q_cols]
    q_buf[pl.ds(other, rows)] = q_far[0, :, q_cols]

    def bring(piece, at, low, high, col):
        to = slice(at, at + high - low)
        k_buf[to] = piece[0, low:high, col : col + heads * DH]
        v_buf[to] = piece[1, low:high, col : col + heads * DH]

    tests = {"side": chip % 2, "core": core}
    for piece, (at, low, high, col, test) in zip(pieces, spots):
        if test is None:
            bring(piece, at, low, high, col)
        else:
            name, wanted = test
            pl.when(tests[name] == wanted)(
                functools.partial(bring, piece, at, low, high, col)
            )

    units = chip_rows // BLK
    factor = SCALE * math.log2(math.e)
    tile_rows = ratio * BLK
    keys_seen = window * BLK
    last = lax.broadcasted_iota(jnp.int32, (BLK, BLK), 1)
    row = lax.broadcasted_iota(jnp.int32, (BLK, BLK), 0)
    causal = jnp.where(last <= row, 0.0, -1e30)
    key = lax.broadcasted_iota(jnp.int32, (8, keys_seen - BLK), 1)
    ones = jnp.ones((keys_seen, DH), jnp.bfloat16)

    def keys_of(unit):
        first_key = base + (unit + 1 - window) * BLK
        return pl.ds(first_key, keys_seen)

    def score(unit, group):
        q_at = pl.ds(unit * BLK, BLK)
        tiles = [
            q_buf[q_at, (group * ratio + s) * DH : (group * ratio + s + 1) * DH]
            for s in range(ratio)
        ]
        s_buf[(unit * heads + group) % SLOTS] = lax.dot_general(
            jnp.concatenate(tiles, axis=0),
            k_buf[keys_of(unit), group * DH : (group + 1) * DH],
            (((1,), (1,)), ((), ())),
            preferred_element_type=jnp.float32,
        )

    def weigh(unit, group):
        number = chip * units + unit
        begin = jnp.int32(0)
        total = jnp.int32(0)
        for doc in range(blocks.shape[0]):
            begin = jnp.where(number >= total, total, begin)
            total = total + blocks[doc]
        hidden = (window - 1 - number + begin) * BLK
        before = jnp.where(key >= hidden, 0.0, -1e30)
        before = jnp.concatenate([before] * (PART // 8), axis=0)
        slot = (unit * heads + group) % SLOTS
        for part in range(tile_rows // PART):
            at = slice(part * PART, (part + 1) * PART)
            low = part * PART % BLK
            bias = jnp.concatenate([before, causal[low : low + PART]], axis=1)
            scores = s_buf[slot, at] * factor + bias
            top = jnp.max(scores, axis=1, keepdims=True)
            w_buf[slot, at] = jnp.exp2(scores - top).astype(jnp.bfloat16)

    def blend(unit, group):
        v_part = v_buf[keys_of(unit), group * DH : (group + 1) * DH]
        blended = jnp.dot(
            w_buf[(unit * heads + group) % SLOTS],
            jnp.concatenate([v_part, ones], axis=1),
            preferred_element_type=jnp.float32,
        )
        blended = (blended[:, :DH] / blended[:, DH:]).astype(jnp.bfloat16)
        for s in range(ratio):
            cols = slice((group * ratio + s) * DH, (group * ratio + s + 1) * DH)
            o_buf[pl.ds(unit * BLK, BLK), cols] = blended[s * BLK : (s + 1) * BLK]

    tiles = [(unit, group) for unit in range(units) for group in range(heads)]
    for step in range(len(tiles) + 2):
        if step < len(tiles):
            score(*tiles[step])
        if 0 <= step - 1 < len(tiles):
            weigh(*tiles[step - 1])
        if 0 <= step - 2:
            blend(*tiles[step - 2])
    out_near[...] = o_buf[pl.ds(mine, rows)]
    out_far[...] = o_buf[pl.ds(other, rows)]
    for store in stores:
        store.wait()


def attend(plan, spots, blocks, q_near, q_far, pieces, puts=(), placed=(), columns=0):
    _, heads, _, ratio, window, spans = plan
    rows = q_near.shape[-2]
    chip_rows = rows * CORES
    held = (spans + 1) * chip_rows
    kv_width = heads * DH
    q_width = kv_width * ratio
    scores = heads * ratio * chip_rows * window * BLK
    scratch_bytes = (chip_rows * q_width + held * kv_width) * 4 + SLOTS * ratio * BLK * window * BLK * 6
    near_by = pl.BlockSpec(memory_space=pltpu.VMEM)
    shape = pltpu.VMEM((rows, q_width), q_near.dtype)
    anywhere = pl.BlockSpec(memory_space=pl.ANY)
    whole = (pltpu.HBM((rows, columns), q_near.dtype),) if puts else ()
    return pl.pallas_call(
        functools.partial(attend_kernel, plan, spots, puts),
        out_shape=(shape, shape) + whole,
        in_specs=[pl.BlockSpec(memory_space=pltpu.SMEM)]
        + [near_by] * (2 + len(pieces))
        + [anywhere] * len(puts),
        out_specs=(near_by, near_by) + (anywhere,) * len(whole),
        scratch_shapes=[
            pltpu.VMEM((chip_rows, q_width), jnp.bfloat16),
            pltpu.VMEM((held, kv_width), jnp.bfloat16),
            pltpu.VMEM((held, kv_width), jnp.bfloat16),
            pltpu.VMEM((chip_rows, q_width), jnp.bfloat16),
            pltpu.VMEM((SLOTS, ratio * BLK, window * BLK), jnp.float32),
            pltpu.VMEM((SLOTS, ratio * BLK, window * BLK), jnp.bfloat16),
        ]
        + [pltpu.SemaphoreType.DMA((len(puts),))] * len(whole),
        cost_estimate=pl.CostEstimate(
            flops=4 * scores * DH,
            bytes_accessed=2 * (chip_rows * q_width * 2 + held * kv_width * 2),
            transcendentals=scores,
        ),
        compiler_params=pltpu.CompilerParams(vmem_limit_bytes=scratch_bytes + (6 << 20)),
    )(blocks, q_near, q_far, *pieces, *placed)


def place_kernel(puts, half, ratio, *refs):
    pieces, out, sems = refs[: len(puts)], refs[-2], refs[-1]
    for store in store_pieces(puts, pieces, out, half, ratio, sems):
        store.wait()


def place(puts, half, ratio, pieces, out):
    anywhere = pl.BlockSpec(memory_space=pl.ANY)
    return pl.pallas_call(
        functools.partial(place_kernel, puts, half, ratio),
        out_shape=pltpu.HBM(out.shape, out.dtype),
        in_specs=[anywhere] * (len(puts) + 1),
        out_specs=anywhere,
        scratch_shapes=[pltpu.SemaphoreType.DMA((len(puts),))],
        input_output_aliases={len(puts): 0},
        compiler_params=pltpu.CompilerParams(vmem_limit_bytes=1 << 20),
        name="place",
    )(*pieces, out)


def split_kernel(arrays, width, early, *refs):
    sources, outs, sems = refs[:arrays], refs[arrays:-1], refs[-1]
    core = lax.axis_index("seq") % CORES
    copies = []
    for out, which, count in zip(
        outs, (1 - core, core, core, 1 - core), (width, width, early, early)
    ):
        for i in range(arrays):
            col = pl.multiple_of(which * width, DH)
            copy = pltpu.make_async_copy(
                sources[i].at[:, pl.ds(col, count)], out.at[i], sems.at[len(copies)]
            )
            copy.start()
            copies.append(copy)
    for copy in copies:
        copy.wait()


def split(early, limit, *arrays):
    rows, columns = arrays[0].shape
    width = columns // CORES
    counts = [width] * 2 + [early] * (2 if early else 0)
    anywhere = pl.BlockSpec(memory_space=pl.ANY)
    return pl.pallas_call(
        functools.partial(split_kernel, len(arrays), width, early),
        out_shape=tuple(
            pltpu.VMEM((len(arrays), rows, count), arrays[0].dtype) for count in counts
        ),
        in_specs=[pl.BlockSpec(memory_space=pltpu.HBM)] * len(arrays),
        out_specs=(anywhere,) * len(counts),
        scratch_shapes=[pltpu.SemaphoreType.DMA((len(counts) * len(arrays),))],
        compiler_params=pltpu.CompilerParams(vmem_limit_bytes=limit),
        name="split",
    )(*arrays)


def merge_kernel(slots, near, far, *outs):
    core = lax.axis_index("seq") % CORES
    rows = near.shape[1]

    def fill(shards):
        for (begin, col), out in zip(slots, outs):
            end = begin + out.shape[1]
            for shard, source in enumerate(shards):
                low, high = max(begin, shard * rows), min(end, (shard + 1) * rows)
                if low < high:
                    out[:, low - begin : high - begin] = source[
                        :, low - shard * rows : high - shard * rows, col : col + out.shape[2]
                    ]

    pl.when(core == 0)(functools.partial(fill, (near, far)))
    pl.when(core == 1)(functools.partial(fill, (far, near)))


def merge(shapes, near, far):
    near_by = pl.BlockSpec(memory_space=pltpu.VMEM)
    slots = tuple((begin, col) for begin, col, _, _ in shapes)
    return pl.pallas_call(
        functools.partial(merge_kernel, slots),
        out_shape=tuple(
            pltpu.VMEM((near.shape[0], count, width), near.dtype)
            for _, _, count, width in shapes
        ),
        in_specs=[near_by, near_by],
        out_specs=(near_by,) * len(shapes),
        compiler_params=pltpu.CompilerParams(vmem_limit_bytes=12 << 20),
        name="merge",
    )(near, far)


def choose_kernel(own, *refs):
    came, out = refs[:-1], refs[-1]
    me = lax.axis_index("seq")
    core = me % CORES
    row = me // CORES % 2

    @pl.when(row == 0)
    def _():
        out[...] = own[...]

    @pl.when(row == 1)
    def _():
        if len(came) == 1:
            out[...] = came[0][...]
        else:
            rows = came[0].shape[1]
            out[:, pl.ds(pl.multiple_of(core * rows, rows), rows)] = came[0][...]
            out[:, pl.ds(pl.multiple_of((1 - core) * rows, rows), rows)] = came[1][...]


def choose(own, *came):
    near_by = pl.BlockSpec(memory_space=pltpu.VMEM)
    return pl.pallas_call(
        choose_kernel,
        out_shape=pltpu.VMEM(own.shape, own.dtype),
        in_specs=[near_by] * (1 + len(came)),
        out_specs=near_by,
        compiler_params=pltpu.CompilerParams(vmem_limit_bytes=6 << 20),
        name="choose",
    )(own, *came)


def chunk_heads(half):
    if half < 6:
        return [1] * half
    return [1, 1] + [2] * ((half - 4) // 2) + [1] * (half % 2 + 2)


def on_device(queries, keys, values, doc_blocks):
    devices = lax.axis_size("seq")
    rows = queries.shape[0]
    q_heads = queries.shape[1] // DH
    kv_heads = keys.shape[1] // DH
    ratio = q_heads // kv_heads
    half = kv_heads // CORES
    chips = devices // CORES
    chip_rows = rows * CORES
    window = rows * devices // BLK // 4
    spans = min(-(-(window - 1) * BLK // chip_rows), chips)

    partner = [(i, i ^ 1) for i in range(devices)]
    next_chip = [(i, i + CORES) for i in range(devices - CORES)]
    next_pair = [(i, (i + 2 * CORES) % devices) for i in range(devices)]
    across = [(i, i ^ CORES) for i in range(devices)]

    sizes = chunk_heads(half)
    firsts = [sum(sizes[:i]) for i in range(len(sizes))]
    base = spans * chip_rows
    lead = base - (window - 1) * BLK
    paired = spans == 2 and chips % 2 == 0 and 0 < lead <= rows and len(sizes) > WHOLE + 1
    crossed = [(i, (i + 2 * CORES) % devices ^ 1) for i in range(devices)]
    early = sizes[0] * DH if paired else 0
    kv_send, kv_near, *firstly = split(early, LIMIT, keys, values)
    kv_far = shift(kv_send, partner)
    if paired:
        straight = shift(firstly[0], next_pair)
        cross = shift(firstly[1], crossed)
    q_send, q_near = split(0, 1 << 20, queries)
    q_far = shift(q_send, partner)

    shapes = []
    for i, (first, heads) in enumerate(zip(firsts, sizes)):
        low = lead if paired and i >= WHOLE else 0
        shapes.append((low, first * DH, chip_rows - low, heads * DH))
    groups = ()
    if paired:
        middle = len(sizes) // 2 + 1
        ends = (firsts[WHOLE], firsts[middle], half)
        groups = tuple(zip(ends, ends[1:]))
        shapes += [(0, low * DH, lead, (high - low) * DH) for low, high in groups]
    merged = merge(shapes, kv_near, kv_far)
    own = merged[: len(sizes)]
    leads, leads_near, leads_far = merged[len(sizes) :], [], []
    for g, block in enumerate(leads):
        leads_near.append(shift(block, across))
        leads_far.append(shift(leads_near[g], next_pair))

    nears, fars = [], []
    for i, (first, heads) in enumerate(zip(firsts, sizes)):
        if paired:
            if i == 0:
                two_back = (straight, cross)
            else:
                two_back = (shift(own[i], next_pair),)
            chosen = choose(own[i], *two_back)
            one_back = shift(chosen, across)
            low = shapes[i][0]
            count = chip_rows - low
            one, two = base - chip_rows, base - 2 * chip_rows
            pieces = [own[i], one_back]
            spots = ((base + low, 0, count, 0, None), (one + low, 0, count, 0, None))
            if i == 0:
                for core, (same, other) in enumerate(((two, two + rows), (two + rows, two))):
                    pieces += [straight, cross]
                    spots += (
                        (same, 0, rows, 0, ("core", core)),
                        (other, 0, rows, 0, ("core", core)),
                    )
            else:
                pieces += [*two_back]
                spots += ((two + low, 0, count, 0, None),)
            if i >= WHOLE:
                g = 0 if i < middle else 1
                pieces += [leads[g], leads_near[g], leads_far[g]]
                col = (first - groups[g][0]) * DH
                spots += (
                    (base, 0, lead, col, None),
                    (one, 0, lead, col, ("side", 1)),
                    (one, 0, lead, col, ("side", 0)),
                )
        else:
            pieces = [own[i]]
            for _ in range(spans):
                pieces.append(shift(pieces[-1], next_chip))
            spots = tuple(
                (base - back * chip_rows, 0, chip_rows, 0, None) for back in range(spans + 1)
            )
        plan = (first, heads, half, ratio, window, spans)
        done, puts = (), ()
        if i == len(sizes) - 1:
            early_far = max(i - 1, 0)
            done = (*nears, *fars[:early_far])
            puts = tuple((0, f) for f in firsts[:i])
            puts += tuple((1, f) for f in firsts[:early_far])
        out_near, out_far, *out = attend(
            plan, spots, doc_blocks, q_near, q_far, pieces, puts, done, queries.shape[1]
        )
        nears.append(out_near)
        fars.append(shift(out_far, partner))
    left = (nears[-1], *fars[early_far:])
    puts = ((0, firsts[-1]), *((1, f) for f in firsts[early_far:]))
    return place(puts, half, ratio, left, out[0])


def solution(mesh):
    spec = P(("groups", "seq"), None)

    return jax.shard_map(
        on_device,
        mesh=mesh,
        in_specs=(spec, spec, spec, P("groups")),
        out_specs=spec,
        check_vma=False,
    )
```

```python
import functools
import math

import jax
import jax.numpy as jnp
from jax import lax
from jax.experimental import pallas as pl
from jax.experimental.pallas import tpu as pltpu
from jax.sharding import PartitionSpec as P


DH = 128
BLK = 128
CORES = 2
SLOTS = 4
WHOLE = 2
LIMIT = 54 << 20
PART = 16
SCALE = 144.0 ** (-0.5)


def shift(block, pairs):
    return lax.ppermute(block, "seq", pairs)


def store_pieces(puts, pieces, out, half, ratio, sems):
    core = lax.axis_index("seq") % CORES
    stores = []
    for (swapped, first), piece in zip(puts, pieces):
        which = 1 - core if swapped else core
        col = pl.multiple_of((which * half + first) * ratio * DH, DH)
        store = pltpu.make_async_copy(
            piece, out.at[:, pl.ds(col, piece.shape[1])], sems.at[len(stores)]
        )
        store.start()
        stores.append(store)
    return stores


def attend_kernel(plan, spots, puts, blocks, q_near, q_far, *rest):
    first, heads, half, ratio, window, spans = plan
    pieces = rest[: len(spots)]
    rest = rest[len(spots) :]
    stores = []
    if puts:
        placed, rest = rest[: len(puts)], rest[len(puts) :]
        out, sems = rest[2], rest[-1]
        rest = rest[:2] + rest[3:-1]
        stores = store_pieces(puts, placed, out, half, ratio, sems)
    out_near, out_far, q_buf, k_buf, v_buf, o_buf, s_buf, w_buf = rest
    rows = q_near.shape[-2]
    chip_rows = rows * CORES
    me = lax.axis_index("seq")
    core = me % CORES
    chip = me // CORES
    q_width = heads * DH * ratio
    base = spans * chip_rows
    q_cols = slice(first * DH * ratio, first * DH * ratio + q_width)
    mine = pl.multiple_of(core * rows, rows)
    other = pl.multiple_of((1 - core) * rows, rows)
    q_buf[pl.ds(mine, rows)] = q_near[0, :, q_cols]
    q_buf[pl.ds(other, rows)] = q_far[0, :, q_cols]

    def bring(piece, at, low, high, col):
        to = slice(at, at + high - low)
        k_buf[to] = piece[0, low:high, col : col + heads * DH]
        v_buf[to] = piece[1, low:high, col : col + heads * DH]

    tests = {"side": chip % 2, "core": core}
    for piece, (at, low, high, col, test) in zip(pieces, spots):
        if test is None:
            bring(piece, at, low, high, col)
        else:
            name, wanted = test
            pl.when(tests[name] == wanted)(
                functools.partial(bring, piece, at, low, high, col)
            )

    units = chip_rows // BLK
    factor = SCALE * math.log2(math.e)
    tile_rows = ratio * BLK
    keys_seen = window * BLK
    last = lax.broadcasted_iota(jnp.int32, (BLK, BLK), 1)
    row = lax.broadcasted_iota(jnp.int32, (BLK, BLK), 0)
    causal = jnp.where(last <= row, 0.0, -1e30)
    key = lax.broadcasted_iota(jnp.int32, (8, keys_seen - BLK), 1)
    ones = jnp.ones((keys_seen, DH), jnp.bfloat16)

    def keys_of(unit):
        first_key = base + (unit + 1 - window) * BLK
        return pl.ds(first_key, keys_seen)

    def score(unit, group):
        q_at = pl.ds(unit * BLK, BLK)
        tiles = [
            q_buf[q_at, (group * ratio + s) * DH : (group * ratio + s + 1) * DH]
            for s in range(ratio)
        ]
        s_buf[(unit * heads + group) % SLOTS] = lax.dot_general(
            jnp.concatenate(tiles, axis=0),
            k_buf[keys_of(unit), group * DH : (group + 1) * DH],
            (((1,), (1,)), ((), ())),
            preferred_element_type=jnp.float32,
        )

    def weigh(unit, group):
        number = chip * units + unit
        begin = jnp.int32(0)
        total = jnp.int32(0)
        for doc in range(blocks.shape[0]):
            begin = jnp.where(number >= total, total, begin)
            total = total + blocks[doc]
        hidden = (window - 1 - number + begin) * BLK
        before = jnp.where(key >= hidden, 0.0, -1e30)
        before = jnp.concatenate([before] * (PART // 8), axis=0)
        slot = (unit * heads + group) % SLOTS
        for part in range(tile_rows // PART):
            at = slice(part * PART, (part + 1) * PART)
            low = part * PART % BLK
            bias = jnp.concatenate([before, causal[low : low + PART]], axis=1)
            scores = s_buf[slot, at] * factor + bias
            top = jnp.max(scores, axis=1, keepdims=True)
            w_buf[slot, at] = jnp.exp2(scores - top).astype(jnp.bfloat16)

    def blend(unit, group):
        v_part = v_buf[keys_of(unit), group * DH : (group + 1) * DH]
        blended = jnp.dot(
            w_buf[(unit * heads + group) % SLOTS],
            jnp.concatenate([v_part, ones], axis=1),
            preferred_element_type=jnp.float32,
        )
        blended = (blended[:, :DH] / blended[:, DH:]).astype(jnp.bfloat16)
        for s in range(ratio):
            cols = slice((group * ratio + s) * DH, (group * ratio + s + 1) * DH)
            o_buf[pl.ds(unit * BLK, BLK), cols] = blended[s * BLK : (s + 1) * BLK]

    tiles = [(unit, group) for unit in range(units) for group in range(heads)]
    for step in range(len(tiles) + 2):
        if step < len(tiles):
            score(*tiles[step])
        if 0 <= step - 1 < len(tiles):
            weigh(*tiles[step - 1])
        if 0 <= step - 2:
            blend(*tiles[step - 2])
    out_near[...] = o_buf[pl.ds(mine, rows)]
    out_far[...] = o_buf[pl.ds(other, rows)]
    for store in stores:
        store.wait()


def attend(plan, spots, blocks, q_near, q_far, pieces, puts=(), placed=(), columns=0):
    _, heads, _, ratio, window, spans = plan
    rows = q_near.shape[-2]
    chip_rows = rows * CORES
    held = (spans + 1) * chip_rows
    kv_width = heads * DH
    q_width = kv_width * ratio
    scores = heads * ratio * chip_rows * window * BLK
    scratch_bytes = (chip_rows * q_width + held * kv_width) * 4 + SLOTS * ratio * BLK * window * BLK * 6
    near_by = pl.BlockSpec(memory_space=pltpu.VMEM)
    shape = pltpu.VMEM((rows, q_width), q_near.dtype)
    anywhere = pl.BlockSpec(memory_space=pl.ANY)
    whole = (pltpu.HBM((rows, columns), q_near.dtype),) if puts else ()
    return pl.pallas_call(
        functools.partial(attend_kernel, plan, spots, puts),
        out_shape=(shape, shape) + whole,
        in_specs=[pl.BlockSpec(memory_space=pltpu.SMEM)]
        + [near_by] * (2 + len(pieces))
        + [anywhere] * len(puts),
        out_specs=(near_by, near_by) + (anywhere,) * len(whole),
        scratch_shapes=[
            pltpu.VMEM((chip_rows, q_width), jnp.bfloat16),
            pltpu.VMEM((held, kv_width), jnp.bfloat16),
            pltpu.VMEM((held, kv_width), jnp.bfloat16),
            pltpu.VMEM((chip_rows, q_width), jnp.bfloat16),
            pltpu.VMEM((SLOTS, ratio * BLK, window * BLK), jnp.float32),
            pltpu.VMEM((SLOTS, ratio * BLK, window * BLK), jnp.bfloat16),
        ]
        + [pltpu.SemaphoreType.DMA((len(puts),))] * len(whole),
        cost_estimate=pl.CostEstimate(
            flops=4 * scores * DH,
            bytes_accessed=2 * (chip_rows * q_width * 2 + held * kv_width * 2),
            transcendentals=scores,
        ),
        compiler_params=pltpu.CompilerParams(vmem_limit_bytes=scratch_bytes + (6 << 20)),
    )(blocks, q_near, q_far, *pieces, *placed)


def place_kernel(puts, half, ratio, *refs):
    pieces, out, sems = refs[: len(puts)], refs[-2], refs[-1]
    for store in store_pieces(puts, pieces, out, half, ratio, sems):
        store.wait()


def place(puts, half, ratio, pieces, out):
    anywhere = pl.BlockSpec(memory_space=pl.ANY)
    return pl.pallas_call(
        functools.partial(place_kernel, puts, half, ratio),
        out_shape=pltpu.HBM(out.shape, out.dtype),
        in_specs=[anywhere] * (len(puts) + 1),
        out_specs=anywhere,
        scratch_shapes=[pltpu.SemaphoreType.DMA((len(puts),))],
        input_output_aliases={len(puts): 0},
        compiler_params=pltpu.CompilerParams(vmem_limit_bytes=1 << 20),
        name="place",
    )(*pieces, out)


def split_kernel(arrays, width, takes, *refs):
    sources, outs, sems = refs[:arrays], refs[arrays:-1], refs[-1]
    core = lax.axis_index("seq") % CORES
    copies = []
    for out, (swapped, count) in zip(outs, takes):
        which = 1 - core if swapped else core
        for i in range(arrays):
            col = pl.multiple_of(which * width, DH)
            copy = pltpu.make_async_copy(
                sources[i].at[:, pl.ds(col, count)], out.at[i], sems.at[len(copies)]
            )
            copy.start()
            copies.append(copy)
    for copy in copies:
        copy.wait()


def split(takes, limit, *arrays):
    rows, columns = arrays[0].shape
    width = columns // CORES
    takes = tuple((swapped, count or width) for swapped, count in takes)
    anywhere = pl.BlockSpec(memory_space=pl.ANY)
    return pl.pallas_call(
        functools.partial(split_kernel, len(arrays), width, takes),
        out_shape=tuple(
            pltpu.VMEM((len(arrays), rows, count), arrays[0].dtype) for _, count in takes
        ),
        in_specs=[pl.BlockSpec(memory_space=pltpu.HBM)] * len(arrays),
        out_specs=(anywhere,) * len(takes),
        scratch_shapes=[pltpu.SemaphoreType.DMA((len(takes) * len(arrays),))],
        compiler_params=pltpu.CompilerParams(vmem_limit_bytes=limit),
        name="split",
    )(*arrays)


def merge_kernel(slots, near, far, *outs):
    core = lax.axis_index("seq") % CORES
    rows = near.shape[1]

    def fill(shards):
        for (begin, col), out in zip(slots, outs):
            end = begin + out.shape[1]
            for shard, source in enumerate(shards):
                low, high = max(begin, shard * rows), min(end, (shard + 1) * rows)
                if low < high:
                    out[:, low - begin : high - begin] = source[
                        :, low - shard * rows : high - shard * rows, col : col + out.shape[2]
                    ]

    pl.when(core == 0)(functools.partial(fill, (near, far)))
    pl.when(core == 1)(functools.partial(fill, (far, near)))


def merge(shapes, near, far):
    near_by = pl.BlockSpec(memory_space=pltpu.VMEM)
    slots = tuple((begin, col) for begin, col, _, _ in shapes)
    return pl.pallas_call(
        functools.partial(merge_kernel, slots),
        out_shape=tuple(
            pltpu.VMEM((near.shape[0], count, width), near.dtype)
            for _, _, count, width in shapes
        ),
        in_specs=[near_by, near_by],
        out_specs=(near_by,) * len(shapes),
        compiler_params=pltpu.CompilerParams(vmem_limit_bytes=12 << 20),
        name="merge",
    )(near, far)


def choose_kernel(own, *refs):
    came, out = refs[:-1], refs[-1]
    me = lax.axis_index("seq")
    core = me % CORES
    row = me // CORES % 2

    @pl.when(row == 0)
    def _():
        out[...] = own[...]

    @pl.when(row == 1)
    def _():
        if len(came) == 1:
            out[...] = came[0][...]
        else:
            rows = came[0].shape[1]
            out[:, pl.ds(pl.multiple_of(core * rows, rows), rows)] = came[0][...]
            out[:, pl.ds(pl.multiple_of((1 - core) * rows, rows), rows)] = came[1][...]


def choose(own, *came):
    near_by = pl.BlockSpec(memory_space=pltpu.VMEM)
    return pl.pallas_call(
        choose_kernel,
        out_shape=pltpu.VMEM(own.shape, own.dtype),
        in_specs=[near_by] * (1 + len(came)),
        out_specs=near_by,
        compiler_params=pltpu.CompilerParams(vmem_limit_bytes=6 << 20),
        name="choose",
    )(own, *came)


def chunk_heads(half):
    if half < 6:
        return [1] * half
    return [1, 1] + [2] * ((half - 4) // 2) + [1] * (half % 2 + 2)


def on_device(queries, keys, values, doc_blocks):
    devices = lax.axis_size("seq")
    rows = queries.shape[0]
    q_heads = queries.shape[1] // DH
    kv_heads = keys.shape[1] // DH
    ratio = q_heads // kv_heads
    half = kv_heads // CORES
    chips = devices // CORES
    chip_rows = rows * CORES
    window = rows * devices // BLK // 4
    spans = min(-(-(window - 1) * BLK // chip_rows), chips)

    partner = [(i, i ^ 1) for i in range(devices)]
    next_chip = [(i, i + CORES) for i in range(devices - CORES)]
    next_pair = [(i, (i + 2 * CORES) % devices) for i in range(devices)]
    across = [(i, i ^ CORES) for i in range(devices)]

    sizes = chunk_heads(half)
    firsts = [sum(sizes[:i]) for i in range(len(sizes))]
    base = spans * chip_rows
    lead = base - (window - 1) * BLK
    paired = spans == 2 and chips % 2 == 0 and 0 < lead <= rows and len(sizes) > WHOLE + 1
    crossed = [(i, (i + 2 * CORES) % devices ^ 1) for i in range(devices)]
    early = sizes[0] * DH if paired else 0
    takes = ((0, early), (1, early)) if paired else ()
    *firstly, kv_send = split((*takes, (1, 0)), LIMIT, keys, values)
    kv_far = shift(kv_send, partner)
    if paired:
        straight = shift(firstly[0], next_pair)
        cross = shift(firstly[1], crossed)
    (kv_near,) = split(((0, 0),), LIMIT, keys, values)
    q_send, q_near = split(((1, 0), (0, 0)), 1 << 20, queries)
    q_far = shift(q_send, partner)

    shapes = []
    for i, (first, heads) in enumerate(zip(firsts, sizes)):
        low = lead if paired and i >= WHOLE else 0
        shapes.append((low, first * DH, chip_rows - low, heads * DH))
    groups = ()
    if paired:
        middle = len(sizes) // 2 + 1
        ends = (firsts[WHOLE], firsts[middle], half)
        groups = tuple(zip(ends, ends[1:]))
        shapes += [(0, low * DH, lead, (high - low) * DH) for low, high in groups]
    merged = merge(shapes, kv_near, kv_far)
    own = merged[: len(sizes)]
    leads, leads_near, leads_far = merged[len(sizes) :], [], []
    for g, block in enumerate(leads):
        leads_near.append(shift(block, across))
        leads_far.append(shift(leads_near[g], next_pair))

    nears, fars = [], []
    for i, (first, heads) in enumerate(zip(firsts, sizes)):
        if paired:
            if i == 0:
                two_back = (straight, cross)
            else:
                two_back = (shift(own[i], next_pair),)
            chosen = choose(own[i], *two_back)
            one_back = shift(chosen, across)
            low = shapes[i][0]
            count = chip_rows - low
            one, two = base - chip_rows, base - 2 * chip_rows
            pieces = [own[i], one_back]
            spots = ((base + low, 0, count, 0, None), (one + low, 0, count, 0, None))
            if i == 0:
                for core, (same, other) in enumerate(((two, two + rows), (two + rows, two))):
                    pieces += [straight, cross]
                    spots += (
                        (same, 0, rows, 0, ("core", core)),
                        (other, 0, rows, 0, ("core", core)),
                    )
            else:
                pieces += [*two_back]
                spots += ((two + low, 0, count, 0, None),)
            if i >= WHOLE:
                g = 0 if i < middle else 1
                pieces += [leads[g], leads_near[g], leads_far[g]]
                col = (first - groups[g][0]) * DH
                spots += (
                    (base, 0, lead, col, None),
                    (one, 0, lead, col, ("side", 1)),
                    (one, 0, lead, col, ("side", 0)),
                )
        else:
            pieces = [own[i]]
            for _ in range(spans):
                pieces.append(shift(pieces[-1], next_chip))
            spots = tuple(
                (base - back * chip_rows, 0, chip_rows, 0, None) for back in range(spans + 1)
            )
        plan = (first, heads, half, ratio, window, spans)
        done, puts = (), ()
        if i == len(sizes) - 1:
            early_far = max(i - 1, 0)
            done = (*nears, *fars[:early_far])
            puts = tuple((0, f) for f in firsts[:i])
            puts += tuple((1, f) for f in firsts[:early_far])
        out_near, out_far, *out = attend(
            plan, spots, doc_blocks, q_near, q_far, pieces, puts, done, queries.shape[1]
        )
        nears.append(out_near)
        fars.append(shift(out_far, partner))
    left = (nears[-1], *fars[early_far:])
    puts = ((0, firsts[-1]), *((1, f) for f in firsts[early_far:]))
    return place(puts, half, ratio, left, out[0])


def solution(mesh):
    spec = P(("groups", "seq"), None)

    return jax.shard_map(
        on_device,
        mesh=mesh,
        in_specs=(spec, spec, spec, P("groups")),
        out_specs=spec,
        check_vma=False,
    )
```
